8 devices in a mesh: dp: 1 (over z), tx: 2 (over y), tyz: 4 (over x, core).
Axes of the slice: x: 2, y: 2, z: 1, core: 2. Of those that a mesh axis runs over, the one named last changes fastest.
Arguments:
- residual: bfloat16 [512, 4096], P('dp', ('tx', 'tyz'))
- ln_scale: bfloat16 [4096], P(('tx', 'tyz'))
- w_query: bfloat16 [4096, 4096], P('tx', 'tyz')
- w_key: bfloat16 [4096, 256], P('tx')
- w_value: bfloat16 [4096, 256], P('tx')
- w_gate: bfloat16 [4096, 16384], P('tx', 'tyz')
- w_up: bfloat16 [4096, 16384], P('tx', 'tyz')
- w_out: bfloat16 [4096, 4096], P('tyz', 'tx')
- w_down: bfloat16 [16384, 4096], P('tyz', 'tx')
- k_cache: bfloat16 [512, 1024, 256], P(('dp', 'tx', 'tyz'))
- v_cache: bfloat16 [512, 1024, 256], P(('dp', 'tx', 'tyz'))
- lengths: int32 [512], P(('dp', 'tx', 'tyz'))
Outputs:
- output 1: bfloat16 [512, 4096], P('dp', ('tx', 'tyz'))
- output 2: bfloat16 [512, 1024, 256], P(('dp', 'tx', 'tyz'))
- output 3: bfloat16 [512, 1024, 256], P(('dp', 'tx', 'tyz'))
All inputs are finite; a program needn't handle non-finite values.
Results may differ from the reference program's by a relative error of at most 0.0142845.
Values are sent between devices in bfloat16 or wider.
A program may use at most 1 GiB of HBM per device.

```python
import jax
import jax.numpy as jnp
from jax import lax

MODEL_DIM = 4096
FF_DIM = 16384
NUM_HEADS = 16
HEAD_DIM = 256
SEQ_LEN = 1024
BATCH_ROWS = 512
ROW_BLOCK = 64
LN_EPS = 1e-5
ROPE_BASE = 10000.0


def draw_lengths(len_key):
    low_key, pick_key = jax.random.split(len_key)
    drawn_lens = jax.random.randint(low_key, (BATCH_ROWS,), SEQ_LEN // 8, SEQ_LEN, dtype=jnp.int32)
    row_order = jax.random.permutation(pick_key, BATCH_ROWS)
    row_ids = jnp.arange(BATCH_ROWS)
    drawn_lens = jnp.where(row_ids == row_order[0], SEQ_LEN - 1, drawn_lens)
    drawn_lens = jnp.where(row_ids == row_order[1], SEQ_LEN // 8, drawn_lens)
    return drawn_lens.astype(jnp.int32)


def setup_inputs(seed: int = 0, part: int = 0) -> dict:
    part_keys = jax.random.split(jax.random.fold_in(jax.random.key(seed), part), 4)
    shared_keys = jax.random.split(jax.random.key(seed + 1), 8)
    q_width = NUM_HEADS * HEAD_DIM
    in_scale = MODEL_DIM ** -0.5
    out_scale = 0.3 * (SEQ_LEN / q_width) ** 0.5
    down_scale = FF_DIM ** -0.5
    return {
        'residual': jax.random.normal(part_keys[0], (BATCH_ROWS, MODEL_DIM), jnp.float32).astype(jnp.bfloat16),
        'ln_scale': (1.0 + 0.4 * jax.random.normal(shared_keys[0], (MODEL_DIM,), jnp.float32)).astype(jnp.bfloat16),
        'w_query': (jax.random.normal(shared_keys[1], (MODEL_DIM, q_width), jnp.float32) * in_scale).astype(jnp.bfloat16),
        'w_key': (jax.random.normal(shared_keys[2], (MODEL_DIM, HEAD_DIM), jnp.float32) * in_scale).astype(jnp.bfloat16),
        'w_value': (jax.random.normal(shared_keys[3], (MODEL_DIM, HEAD_DIM), jnp.float32) * in_scale).astype(jnp.bfloat16),
        'w_gate': (jax.random.normal(shared_keys[4], (MODEL_DIM, FF_DIM), jnp.float32) * in_scale).astype(jnp.bfloat16),
        'w_up': (jax.random.normal(shared_keys[5], (MODEL_DIM, FF_DIM), jnp.float32) * in_scale).astype(jnp.bfloat16),
        'w_out': (jax.random.normal(shared_keys[6], (q_width, MODEL_DIM), jnp.float32) * out_scale).astype(jnp.bfloat16),
        'w_down': (jax.random.normal(shared_keys[7], (FF_DIM, MODEL_DIM), jnp.float32) * down_scale).astype(jnp.bfloat16),
        'k_cache': jax.random.normal(part_keys[1], (BATCH_ROWS, SEQ_LEN, HEAD_DIM), jnp.float32).astype(jnp.bfloat16),
        'v_cache': jax.random.normal(part_keys[2], (BATCH_ROWS, SEQ_LEN, HEAD_DIM), jnp.float32).astype(jnp.bfloat16),
        'lengths': draw_lengths(part_keys[3]),
    }


def rope_rotate(vectors, positions):
    head_dim = vectors.shape[-1]
    half_dim = head_dim // 2
    inv_freq = ROPE_BASE ** (-2.0 * jnp.arange(half_dim, dtype=jnp.float32) / head_dim)
    angles = positions.astype(jnp.float32)[:, None] * inv_freq[None, :]
    bcast_shape = (angles.shape[0],) + (1,) * (vectors.ndim - 2) + (half_dim,)
    cos_part = jnp.cos(angles).reshape(bcast_shape)
    sin_part = jnp.sin(angles).reshape(bcast_shape)
    vec_f32 = vectors.astype(jnp.float32)
    first_half = vec_f32[..., :half_dim]
    second_half = vec_f32[..., half_dim:]
    rotated = jnp.concatenate([first_half * cos_part - second_half * sin_part, second_half * cos_part + first_half * sin_part], axis=-1)
    return rotated.astype(jnp.bfloat16)


def attend_rows(query_rot, key_rot, value_new, k_cache, v_cache, lengths):
    positions = jnp.arange(k_cache.shape[1], dtype=jnp.int32)
    write_mask = (positions[None, :] == lengths[:, None])[:, :, None]
    k_updated = jnp.where(write_mask, key_rot[:, None, :], k_cache)
    v_updated = jnp.where(write_mask, value_new[:, None, :], v_cache)
    scores = jnp.einsum('rhd,rtd->rht', query_rot.astype(jnp.float32), k_updated.astype(jnp.float32)) * (query_rot.shape[-1] ** -0.5)
    valid_mask = (positions[None, :] <= lengths[:, None])[:, None, :]
    scores = jnp.where(valid_mask, scores, -1e30)
    attn_probs = jax.nn.softmax(scores, axis=-1).astype(jnp.bfloat16)
    attended = jnp.einsum('rht,rtd->rhd', attn_probs.astype(jnp.float32), v_updated.astype(jnp.float32)).astype(jnp.bfloat16)
    return attended, k_updated, v_updated


def reference(residual, ln_scale, w_query, w_key, w_value, w_gate, w_up, w_out, w_down, k_cache, v_cache, lengths):
    res_f32 = residual.astype(jnp.float32)
    row_mean = jnp.mean(res_f32, axis=-1, keepdims=True)
    row_var = jnp.mean(jnp.square(res_f32 - row_mean), axis=-1, keepdims=True)
    normed = ((res_f32 - row_mean) * lax.rsqrt(row_var + LN_EPS) * ln_scale.astype(jnp.float32)).astype(jnp.bfloat16)
    query_vec = jnp.dot(normed, w_query, preferred_element_type=jnp.float32).astype(jnp.bfloat16)
    key_new = jnp.dot(normed, w_key, preferred_element_type=jnp.float32).astype(jnp.bfloat16)
    value_new = jnp.dot(normed, w_value, preferred_element_type=jnp.float32).astype(jnp.bfloat16)
    gate_val = jnp.dot(normed, w_gate, preferred_element_type=jnp.float32).astype(jnp.bfloat16)
    up_val = jnp.dot(normed, w_up, preferred_element_type=jnp.float32).astype(jnp.bfloat16)
    mlp_act = (jax.nn.silu(gate_val.astype(jnp.float32)) * up_val.astype(jnp.float32)).astype(jnp.bfloat16)
    query_rot = rope_rotate(query_vec.reshape(BATCH_ROWS, NUM_HEADS, HEAD_DIM), lengths)
    key_rot = rope_rotate(key_new, lengths)
    num_blocks = BATCH_ROWS // ROW_BLOCK

    def attend_block(block_args):
        return attend_rows(block_args[0], block_args[1], block_args[2], block_args[3], block_args[4], block_args[5])

    attended, k_blocks, v_blocks = lax.map(attend_block, (
        query_rot.reshape(num_blocks, ROW_BLOCK, NUM_HEADS, HEAD_DIM),
        key_rot.reshape(num_blocks, ROW_BLOCK, HEAD_DIM),
        value_new.reshape(num_blocks, ROW_BLOCK, HEAD_DIM),
        k_cache.reshape(num_blocks, ROW_BLOCK, SEQ_LEN, HEAD_DIM),
        v_cache.reshape(num_blocks, ROW_BLOCK, SEQ_LEN, HEAD_DIM),
        lengths.reshape(num_blocks, ROW_BLOCK)))
    attn_flat = attended.reshape(BATCH_ROWS, NUM_HEADS * HEAD_DIM)
    block_out = jnp.dot(attn_flat, w_out, preferred_element_type=jnp.float32) + jnp.dot(mlp_act, w_down, preferred_element_type=jnp.float32)
    new_resid = (res_f32 + block_out).astype(jnp.bfloat16)
    return (new_resid, k_blocks.reshape(BATCH_ROWS, SEQ_LEN, HEAD_DIM), v_blocks.reshape(BATCH_ROWS, SEQ_LEN, HEAD_DIM))
```

```python
import functools

import jax
import jax.numpy as jnp
from jax import lax
from jax.experimental import pallas as pl
from jax.experimental.pallas import tpu as pltpu
from jax.sharding import PartitionSpec as P

LN_EPS = 1e-5
ROPE_BASE = 10000.0
MESH = pl.DeviceIdType.MESH
F32 = jnp.float32
BF16 = jnp.bfloat16
GATHER_CHUNKS = 4
ATTN_ROWS = 4


def gather_kernel(res_ref, stat_ref, ln_ref, raw_ref, stats_ref, lns_ref,
                  stat_send, stat_recv, ln_send, ln_recv, pair_send, pair_recv,
                  x_send, x_recv, relay_send, relay_recv):
    tx = lax.axis_index('tx')
    ty = lax.axis_index('tyz')
    rows, width = res_ref.shape
    chunk = rows // GATHER_CHUNKS
    pair = ty + 1 - 2 * lax.rem(ty, 2)
    across = lax.rem(ty + 2, 4)
    me = tx * 4 + ty
    barrier = pltpu.get_barrier_semaphore()
    for off in range(1, 8):
        peer = lax.rem(me + off, 8)
        pl.semaphore_signal(barrier, inc=1, device_id={'tx': peer // 4, 'tyz': lax.rem(peer, 4)}, device_id_type=MESH)
    pl.semaphore_wait(barrier, 7)

    def cols(who):
        return pl.ds(pl.multiple_of(who * width, width), width)

    copies = []
    for off in range(1, 8):
        peer = lax.rem(me + off, 8)
        copies.append(pltpu.make_async_remote_copy(
            stat_ref, stats_ref.at[me], stat_send.at[off], stat_recv.at[off],
            device_id={'tx': peer // 4, 'tyz': lax.rem(peer, 4)}, device_id_type=MESH))
    for off in range(1, 4):
        peer = lax.rem(ty + off, 4)
        copies.append(pltpu.make_async_remote_copy(
            ln_ref, lns_ref.at[:, cols(ty)], ln_send.at[off], ln_recv.at[off],
            device_id={'tyz': peer}, device_id_type=MESH))
    for copy in copies:
        copy.start()
    crossing = []
    for idx in range(GATHER_CHUNKS):
        block = pl.ds(idx * chunk, chunk)
        copy = pltpu.make_async_remote_copy(
            res_ref.at[block], raw_ref.at[block, cols(ty)], x_send.at[idx], x_recv.at[idx],
            device_id={'tyz': across}, device_id_type=MESH)
        copy.start()
        crossing.append(copy)
    copy = pltpu.make_async_remote_copy(
        res_ref, raw_ref.at[:, cols(ty)], pair_send, pair_recv,
        device_id={'tyz': pair}, device_id_type=MESH)
    copy.start()
    copies.append(copy)
    raw_ref[:, cols(ty)] = res_ref[...]
    stats_ref[me] = stat_ref[...]
    lns_ref[:, cols(ty)] = ln_ref[...]
    for idx in range(GATHER_CHUNKS):
        block = pl.ds(idx * chunk, chunk)
        crossing[idx].wait_recv()
        copy = pltpu.make_async_remote_copy(
            raw_ref.at[block, cols(across)], raw_ref.at[block, cols(across)],
            relay_send.at[idx], relay_recv.at[idx], device_id={'tyz': pair}, device_id_type=MESH)
        copy.start()
        copies.append(copy)
    for copy in crossing:
        copy.wait_send()
    for copy in copies:
        copy.wait()


def gather_inputs(residual, stat, ln_scale):
    rows, width = residual.shape
    dma = pltpu.SemaphoreType.DMA
    vmem = pl.BlockSpec(memory_space=pltpu.VMEM)
    return pl.pallas_call(
        gather_kernel,
        out_shape=(jax.ShapeDtypeStruct((rows, width * 4), residual.dtype),
                   jax.ShapeDtypeStruct((8,) + stat.shape, stat.dtype),
                   jax.ShapeDtypeStruct((16, width * 4), ln_scale.dtype)),
        in_specs=[vmem] * 3,
        out_specs=(vmem,) * 3,
        scratch_shapes=[dma((8,)), dma((8,)), dma((4,)), dma((4,)), dma, dma,
                        dma((GATHER_CHUNKS,)), dma((GATHER_CHUNKS,)), dma((GATHER_CHUNKS,)), dma((GATHER_CHUNKS,))],
        compiler_params=pltpu.CompilerParams(collective_id=0, has_side_effects=True),
        cost_estimate=pl.CostEstimate(flops=2 ** 31, bytes_accessed=2 ** 22, transcendentals=0),
        name='gather_inputs',
    )(residual, stat, jnp.broadcast_to(ln_scale[None, :], (16, width)))


def attend_kernel(len_ref, q_ref, knew_ref, vnew_ref, kc_ref, vc_ref, o_ref, kout_ref, vout_ref):
    step = pl.program_id(0)
    rows = q_ref.shape[0]
    seq = kc_ref.shape[1]
    scale = q_ref.shape[2] ** -0.5
    for row in range(rows):
        pos = len_ref[step * rows + row]
        start = pl.multiple_of((pos // 16) * 16, 16)
        hit = lax.broadcasted_iota(jnp.int32, (16, 1), 0) == pos - start
        for cache, new, out in ((kc_ref, knew_ref, kout_ref), (vc_ref, vnew_ref, vout_ref)):
            out[row] = cache[row]
            window = cache[row, pl.ds(start, 16), :].astype(F32)
            out[row, pl.ds(start, 16), :] = jnp.where(hit, new[row].astype(F32), window).astype(BF16)
    for row in range(rows):
        pos = len_ref[step * rows + row]
        scores = lax.dot_general(q_ref[row], kout_ref[row], (((1,), (1,)), ((), ())), preferred_element_type=F32) * scale
        where = lax.broadcasted_iota(jnp.int32, (1, seq), 1) <= pos
        scores = jnp.where(where, scores, -1e30)
        top = jnp.max(scores, axis=1, keepdims=True)
        weight = jnp.exp(scores - top)
        probs = (weight / jnp.sum(weight, axis=1, keepdims=True)).astype(BF16)
        o_ref[row] = jnp.dot(probs, vout_ref[row], preferred_element_type=F32).astype(BF16)


def attend(lengths, query, key_new, value_new, k_cache, v_cache):
    rows, heads, dim = query.shape
    seq = k_cache.shape[1]
    small = pl.BlockSpec((ATTN_ROWS, heads, dim), lambda i, lens: (i, 0, 0))
    new = pl.BlockSpec((ATTN_ROWS, 1, dim), lambda i, lens: (i, 0, 0))
    big = pl.BlockSpec((ATTN_ROWS, seq, dim), lambda i, lens: (i, 0, 0))
    return pl.pallas_call(
        attend_kernel,
        grid_spec=pltpu.PrefetchScalarGridSpec(
            num_scalar_prefetch=1, grid=(rows // ATTN_ROWS,),
            in_specs=[small, new, new, big, big], out_specs=[small, big, big]),
        out_shape=(jax.ShapeDtypeStruct(query.shape, BF16),
                   jax.ShapeDtypeStruct(k_cache.shape, BF16),
                   jax.ShapeDtypeStruct(v_cache.shape, BF16)),
        compiler_params=pltpu.CompilerParams(vmem_limit_bytes=40 * 2 ** 20),
        cost_estimate=pl.CostEstimate(flops=2 ** 33, bytes_accessed=2 ** 27, transcendentals=2 ** 20),
        name='attend',
    )(lengths, query, key_new[:, None, :], value_new[:, None, :], k_cache, v_cache)


def scatter_kernel(part_ref, res_ref, out_ref, recv, send_sem, recv_sem):
    ty = lax.axis_index('tyz')
    width = out_ref.shape[1]
    barrier = pltpu.get_barrier_semaphore()
    for off in range(1, 4):
        pl.semaphore_signal(barrier, inc=1, device_id={'tyz': lax.rem(ty + off, 4)}, device_id_type=MESH)
    pl.semaphore_wait(barrier, 3)
    copies = []
    for off in (2, 1, 3):
        peer = lax.rem(ty + off, 4)
        copy = pltpu.make_async_remote_copy(
            part_ref.at[:, pl.ds(pl.multiple_of(peer * width, width), width)], recv.at[off],
            send_sem.at[off], recv_sem.at[off], device_id={'tyz': peer}, device_id_type=MESH)
        copy.start()
        copies.append(copy)
    total = part_ref[:, pl.ds(pl.multiple_of(ty * width, width), width)].astype(F32)
    for copy in copies:
        copy.wait()
    for off in range(1, 4):
        total = total + recv[off].astype(F32)
    out_ref[...] = (res_ref[...].astype(F32) + total).astype(out_ref.dtype)


def scatter_sum(part, residual):
    dma = pltpu.SemaphoreType.DMA
    vmem = pl.BlockSpec(memory_space=pltpu.VMEM)
    return pl.pallas_call(
        scatter_kernel,
        out_shape=jax.ShapeDtypeStruct(residual.shape, residual.dtype),
        in_specs=[vmem] * 2,
        out_specs=vmem,
        scratch_shapes=[pltpu.VMEM((4,) + residual.shape, BF16), dma((4,)), dma((4,))],
        compiler_params=pltpu.CompilerParams(collective_id=1, has_side_effects=True),
        cost_estimate=pl.CostEstimate(flops=2 ** 30, bytes_accessed=2 ** 22, transcendentals=0),
        name='scatter_sum',
    )(part, residual)


def solution(mesh):
    tx_size = mesh.shape['tx']
    tyz_size = mesh.shape['tyz']
    row_axes = ('dp', 'tx', 'tyz')
    swap = [(0, 1), (1, 0)]

    def rotate(vectors, cos_part, sin_part):
        half = vectors.shape[-1] // 2
        first = vectors[..., :half].astype(F32)
        second = vectors[..., half:].astype(F32)
        return jnp.concatenate([first * cos_part - second * sin_part, second * cos_part + first * sin_part], axis=-1).astype(BF16)

    def decode_layer(residual, ln_scale, w_query, w_key, w_value, w_gate, w_up, w_out, w_down, k_cache, v_cache, lengths):
        tx = lax.axis_index('tx')
        ty = lax.axis_index('tyz')
        rows, width = residual.shape
        half = rows // tx_size
        model_dim = width * tx_size * tyz_size
        rows_local = k_cache.shape[0]
        head_dim = w_key.shape[1]
        lanes = 128

        def dot(a, b):
            return jnp.dot(a, b, preferred_element_type=F32)

        res_f32 = residual.astype(F32)
        row_sum = jnp.sum(res_f32, axis=1)
        row_sq = jnp.sum(jnp.square(res_f32 - (row_sum / width)[:, None]), axis=1)
        stat = jnp.concatenate([row_sum.reshape(rows // lanes, lanes), row_sq.reshape(rows // lanes, lanes)], axis=0)
        raw, stats, lns = gather_inputs(residual, stat, ln_scale)
        sums = stats[:, :rows // lanes].reshape(-1, rows)
        sqs = stats[:, rows // lanes:].reshape(-1, rows)
        mean = jnp.sum(sums, axis=0) / model_dim
        var = jnp.sum(sqs + width * jnp.square(sums / width - mean), axis=0) / model_dim
        normed = ((raw.astype(F32) - mean[:, None]) * lax.rsqrt(var + LN_EPS)[:, None] * lns[0].astype(F32)).astype(BF16)
        mine = lax.dynamic_slice_in_dim(normed, tx * half, half, axis=0)
        other = lax.dynamic_slice_in_dim(normed, (1 - tx) * half, half, axis=0)

        def pass_on(x):
            return lax.ppermute(x, 'tx', swap)

        query_got = pass_on(dot(other, w_query).astype(BF16))
        other_few = lax.dynamic_slice_in_dim(other, ty * rows_local, rows_local, axis=0)
        mine_few = lax.dynamic_slice_in_dim(mine, ty * rows_local, rows_local, axis=0)
        kv_got = pass_on(jnp.concatenate([dot(other_few, w_key), dot(other_few, w_value)], axis=1).astype(BF16))
        gate_other = dot(other, w_gate).astype(BF16)
        up_other = dot(other, w_up).astype(BF16)
        blocks = 4
        size = half // blocks
        gate_got = []
        up_got = []
        for idx in range(blocks):
            gate_got.append(pass_on(gate_other[idx * size:(idx + 1) * size]))
            up_got.append(pass_on(up_other[idx * size:(idx + 1) * size]))
        query_rows = (dot(mine, w_query) + query_got.astype(F32)).astype(BF16)
        key_new = (dot(mine_few, w_key) + kv_got[:, :head_dim].astype(F32)).astype(BF16)
        value_new = (dot(mine_few, w_value) + kv_got[:, head_dim:].astype(F32)).astype(BF16)
        gate_mine = dot(mine, w_gate).astype(BF16)
        up_mine = dot(mine, w_up).astype(BF16)

        half_dim = head_dim // 2
        inv_freq = ROPE_BASE ** (-2.0 * jnp.arange(half_dim, dtype=F32) / head_dim)
        angles = lengths.astype(F32)[:, None] * inv_freq[None, :]
        cos_part = jnp.cos(angles)
        sin_part = jnp.sin(angles)
        query_mine = lax.all_to_all(query_rows.reshape(half, -1, head_dim), 'tyz', 0, 1, tiled=True)
        query_rot = rotate(query_mine, cos_part[:, None], sin_part[:, None])
        key_rot = rotate(key_new, cos_part, sin_part)
        query_rot, gate_mine, up_mine = lax.optimization_barrier((query_rot, gate_mine, up_mine))
        attended, k_updated, v_updated = attend(lengths, query_rot, key_rot, value_new, k_cache, v_cache)
        attended_mine = lax.all_to_all(attended, 'tyz', 1, 0, tiled=True).reshape(half, -1)
        attended_other = pass_on(attended_mine)

        acts = []
        acts_got = []
        for idx in range(blocks):
            gate = gate_mine[idx * size:(idx + 1) * size].astype(F32) + gate_got[idx].astype(F32)
            up = up_mine[idx * size:(idx + 1) * size].astype(F32) + up_got[idx].astype(F32)
            gate = gate.astype(BF16).astype(F32)
            up = up.astype(BF16).astype(F32)
            act = (jax.nn.silu(gate) * up).astype(BF16)
            acts.append(act)
            acts_got.append(pass_on(act))
        part_mine = dot(attended_mine, w_out) + dot(jnp.concatenate(acts, axis=0), w_down)
        res_mine = lax.dynamic_slice_in_dim(residual, tx * half, half, axis=0)
        res_other = lax.dynamic_slice_in_dim(residual, (1 - tx) * half, half, axis=0)
        out_mine = scatter_sum(part_mine.astype(BF16), res_mine)
        part_other = dot(attended_other, w_out) + dot(jnp.concatenate(acts_got, axis=0), w_down)
        out_other = scatter_sum(part_other.astype(BF16), res_other)
        new_resid = jnp.where(tx == 0, jnp.concatenate([out_mine, out_other]), jnp.concatenate([out_other, out_mine]))
        return new_resid, k_updated, v_updated

    in_specs = (P('dp', ('tx', 'tyz')), P(('tx', 'tyz')), P('tx', 'tyz'), P('tx', None), P('tx', None), P('tx', 'tyz'), P('tx', 'tyz'), P('tyz', 'tx'), P('tyz', 'tx'), P(row_axes, None, None), P(row_axes, None, None), P(row_axes))
    out_specs = (P('dp', ('tx', 'tyz')), P(row_axes, None, None), P(row_axes, None, None))
    return jax.shard_map(decode_layer, mesh=mesh, in_specs=in_specs, out_specs=out_specs, check_vma=False)
```

```python
import functools

import jax
import jax.numpy as jnp
from jax import lax
from jax.experimental import pallas as pl
from jax.experimental.pallas import tpu as pltpu
from jax.sharding import PartitionSpec as P

LN_EPS = 1e-5
ROPE_BASE = 10000.0
MESH = pl.DeviceIdType.MESH
F32 = jnp.float32
BF16 = jnp.bfloat16
CHUNKS = 4
SLOTS = 4
WCOLS = 512
ATTN_ROWS = 4


def front_kernel(res_ref, ln_ref, wq_ref, wk_ref, wv_ref, wg_ref, wu_ref,
                 gu0_ref, gu1_ref, gu2_ref, gu3_ref, mine_ref, q_ref, k_ref, v_ref,
                 raw, hn, wq, wkv, slots, stage, stat, stats, lnb, lns, colstat, q_send, q_got, q_own, kv_send, kv_got,
                 stat_send, stat_recv, ln_send, ln_recv, pair_send, pair_recv, x_send, x_recv, relay_send, relay_recv,
                 q_ssem, q_rsem, kv_ssem, kv_rsem, wq_sem, slot_sem, out_sem):
    tx = lax.axis_index('tx')
    ty = lax.axis_index('tyz')
    rows, width = res_ref.shape
    half = rows // 2
    model_dim = 8 * width
    chunk = rows // CHUNKS
    pair = ty + 1 - 2 * lax.rem(ty, 2)
    across = lax.rem(ty + 2, 4)
    me = tx * 4 + ty
    few = k_ref.shape[0]
    dim = k_ref.shape[1]
    wcols = slots.shape[2]
    ff = wg_ref.shape[1]
    per = ff // wcols

    def dot(a, b):
        return jnp.dot(a, b, preferred_element_type=F32)

    weights = [pltpu.make_async_copy(wq_ref, wq, wq_sem.at[0]),
               pltpu.make_async_copy(wk_ref, wkv.at[:, pl.ds(0, dim)], wq_sem.at[1]),
               pltpu.make_async_copy(wv_ref, wkv.at[:, pl.ds(dim, dim)], wq_sem.at[2])]
    for copy in weights:
        copy.start()

    def fetch(ref, idx, slot):
        start = pl.multiple_of(idx * wcols, wcols)
        return pltpu.make_async_copy(ref.at[:, pl.ds(start, wcols)], slots.at[slot], slot_sem.at[slot])

    for idx in range(SLOTS - 1):
        fetch(wg_ref, idx, idx).start()

    barrier = pltpu.get_barrier_semaphore()
    for off in range(1, 8):
        peer = lax.rem(me + off, 8)
        pl.semaphore_signal(barrier, inc=1, device_id={'tx': peer // 4, 'tyz': lax.rem(peer, 4)}, device_id_type=MESH)
    lnb[...] = jnp.broadcast_to(ln_ref[...], lnb.shape)
    pl.semaphore_wait(barrier, 7)

    def cols(who):
        return pl.ds(pl.multiple_of(who * width, width), width)

    def actual(idx):
        start = (1 - tx) * half + idx * chunk if idx < CHUNKS // 2 else tx * half + idx * chunk - half
        return pl.ds(pl.multiple_of(start, chunk), chunk)

    def block(idx):
        return pl.ds(idx * chunk, chunk)

    copies = []
    crossing = []
    paired = []
    relayed = []
    for idx in range(CHUNKS):
        crossing.append(pltpu.make_async_remote_copy(
            res_ref.at[actual(idx)], raw.at[block(idx), cols(ty)], x_send.at[idx], x_recv.at[idx],
            device_id={'tyz': across}, device_id_type=MESH))
        paired.append(pltpu.make_async_remote_copy(
            res_ref.at[actual(idx)], raw.at[block(idx), cols(ty)], pair_send.at[idx], pair_recv.at[idx],
            device_id={'tyz': pair}, device_id_type=MESH))
        relayed.append(pltpu.make_async_remote_copy(
            raw.at[block(idx), cols(across)], raw.at[block(idx), cols(across)], relay_send.at[idx], relay_recv.at[idx],
            device_id={'tyz': pair}, device_id_type=MESH))
    crossing[0].start()
    paired[0].start()

    res = res_ref[...].astype(F32)
    row_sum = jnp.sum(res, axis=1, keepdims=True)
    row_sq = jnp.sum(jnp.square(res - row_sum / width), axis=1, keepdims=True)
    lane = lax.broadcasted_iota(jnp.int32, (rows, 128), 1)
    both = jnp.where(lax.rem(lane, 8) < 4, row_sum, row_sq)
    stat[...] = both.T[:8]
    for idx in range(CHUNKS):
        raw[block(idx), cols(ty)] = res_ref[actual(idx), :]
    lns[:, cols(ty)] = lnb[...]
    stats[me] = stat[...]
    for off in range(1, 8):
        peer = lax.rem(me + off, 8)
        copies.append(pltpu.make_async_remote_copy(
            stat, stats.at[me], stat_send.at[off], stat_recv.at[off],
            device_id={'tx': peer // 4, 'tyz': lax.rem(peer, 4)}, device_id_type=MESH))
    for off in range(1, 4):
        copies.append(pltpu.make_async_remote_copy(
            lnb, lns.at[:, cols(ty)], ln_send.at[off], ln_recv.at[off],
            device_id={'tyz': lax.rem(ty + off, 4)}, device_id_type=MESH))
    for copy in copies:
        copy.start()
    for idx in range(1, CHUNKS):
        crossing[idx].start()
        paired[idx].start()
    for copy in copies:
        copy.wait_recv()
    total = stats[0][:1]
    for src in range(1, 8):
        total = total + stats[src][:1]
    mean = total / model_dim
    square = jnp.zeros_like(mean)
    for src in range(8):
        square = square + stats[src][4:5] + width * jnp.square(stats[src][:1] / width - mean)
    scale = lax.rsqrt(square / model_dim + LN_EPS)
    upper = lax.broadcasted_iota(jnp.int32, (128, rows), 0) < 64
    cstat = jnp.where(upper, mean, scale).T
    start_mine = pl.multiple_of(tx * half, half)
    start_other = pl.multiple_of((1 - tx) * half, half)
    colstat[...] = cstat

    def norm(idx):
        centre = colstat[actual(idx), :][:, :1]
        factor = colstat[actual(idx), :][:, 64:65]
        for col in range(4):
            part = pl.ds(col * width, width)
            hn[block(idx), part] = ((raw[block(idx), part].astype(F32) - centre) * factor
                                    * lns[:1, part].astype(F32)).astype(BF16)

    q_copies = []
    for idx in range(CHUNKS // 2):
        crossing[idx].wait_recv()
        relayed[idx].start()
        paired[idx].wait_recv()
        relayed[idx].wait_recv()
        norm(idx)
        if idx == 0:
            weights[0].wait()
        q_send[block(idx), :] = dot(hn[block(idx), :], wq[...]).astype(BF16)
        copy = pltpu.make_async_remote_copy(
            q_send.at[block(idx)], q_got.at[block(idx)], q_ssem.at[idx], q_rsem.at[idx],
            device_id={'tx': 1 - tx}, device_id_type=MESH)
        copy.start()
        q_copies.append(copy)
    weights[1].wait()
    weights[2].wait()
    mine_few = pl.ds(pl.multiple_of(ty * few, few), few)
    kv_send[...] = dot(hn[mine_few, :], wkv[...]).astype(BF16)
    kv_copy = pltpu.make_async_remote_copy(kv_send, kv_got, kv_ssem, kv_rsem, device_id={'tx': 1 - tx}, device_id_type=MESH)
    kv_copy.start()

    outs = (gu0_ref, gu1_ref, gu2_ref, gu3_ref)
    size = half // len(outs)

    def put(step, slot):
        start = pl.multiple_of(step * wcols, wcols)
        return [pltpu.make_async_copy(stage.at[slot, pl.ds(idx * size, size)], out.at[:, pl.ds(start, wcols)], out_sem.at[slot, idx])
                for idx, out in enumerate(outs)]

    def body(step, carry, first):
        slot = lax.rem(step, SLOTS)
        side = lax.rem(step, 2)
        ahead = step + SLOTS - 1
        into = lax.rem(ahead, SLOTS)
        if first:
            @pl.when(ahead < per)
            def _():
                fetch(wg_ref, ahead, into).start()

            @pl.when(ahead >= per)
            def _():
                fetch(wu_ref, ahead - per, into).start()
            fetch(wg_ref, 0, slot).wait()
        else:
            @pl.when(ahead < 2 * per)
            def _():
                fetch(wu_ref, ahead - per, into).start()
            fetch(wu_ref, 0, slot).wait()

        @pl.when(step >= 2)
        def _():
            for copy in put(step - 2, side):
                copy.wait()
        stage[side] = dot(hn[:half, :], slots[slot]).astype(BF16)
        for copy in put(step, side):
            copy.start()
        return carry

    lax.fori_loop(0, per, functools.partial(body, first=True), 0)
    for idx in range(CHUNKS // 2, CHUNKS):
        crossing[idx].wait_recv()
        relayed[idx].start()
    for idx in range(CHUNKS // 2, CHUNKS):
        paired[idx].wait_recv()
        relayed[idx].wait_recv()
        norm(idx)
    q_own[...] = dot(hn[half:, :], wq[...]).astype(BF16)
    mine_ref[...] = hn[half:, :]
    own_few = pl.ds(pl.multiple_of(half + ty * few, few), few)
    kv_own = dot(hn[own_few, :], wkv[...])
    lax.fori_loop(per, 2 * per, functools.partial(body, first=False), 0)
    kv_copy.wait()
    kv = (kv_own + kv_got[...].astype(F32)).astype(BF16)
    k_ref[...] = kv[:, :dim]
    v_ref[...] = kv[:, dim:]
    for copy in q_copies:
        copy.wait()
    q_ref[...] = (q_own[...].astype(F32) + q_got[...].astype(F32)).astype(BF16)
    for copy in copies + crossing + paired + relayed:
        copy.wait_send()
    for step in (2 * per - 2, 2 * per - 1):
        for copy in put(step, step % 2):
            copy.wait()


def front(residual, ln_scale, w_query, w_key, w_value, w_gate, w_up, few):
    rows, width = residual.shape
    half = rows // 2
    depth, q_cols = w_query.shape
    dim = w_key.shape[1]
    ff = w_gate.shape[1]
    dma = pltpu.SemaphoreType.DMA
    vmem = pl.BlockSpec(memory_space=pltpu.VMEM)
    hbm = pl.BlockSpec(memory_space=pl.ANY)
    shape = jax.ShapeDtypeStruct
    size = half // 4
    return pl.pallas_call(
        front_kernel,
        out_shape=(shape((size, 2 * ff), BF16),) * 4 + (shape((half, depth), BF16), shape((half, q_cols), BF16),
                                                      shape((few, dim), BF16), shape((few, dim), BF16)),
        in_specs=[vmem] * 2 + [hbm] * 5,
        out_specs=(hbm,) * 4 + (vmem,) * 4,
        scratch_shapes=[
            pltpu.VMEM((rows, depth), BF16), pltpu.VMEM((rows, depth), BF16),
            pltpu.VMEM((depth, q_cols), BF16), pltpu.VMEM((depth, 2 * dim), BF16),
            pltpu.VMEM((SLOTS, depth, WCOLS), BF16), pltpu.VMEM((2, half, WCOLS), BF16),
            pltpu.VMEM((8, rows), F32), pltpu.VMEM((8, 8, rows), F32),
            pltpu.VMEM((16, width), BF16), pltpu.VMEM((16, depth), BF16), pltpu.VMEM((rows, 128), F32),
            pltpu.VMEM((half, q_cols), BF16), pltpu.VMEM((half, q_cols), BF16), pltpu.VMEM((half, q_cols), BF16),
            pltpu.VMEM((few, 2 * dim), BF16), pltpu.VMEM((few, 2 * dim), BF16),
            dma((8,)), dma((8,)), dma((4,)), dma((4,)), dma((CHUNKS,)), dma((CHUNKS,)), dma((CHUNKS,)), dma((CHUNKS,)),
            dma((CHUNKS,)), dma((CHUNKS,)), dma((CHUNKS,)), dma((CHUNKS,)), dma, dma, dma((3,)), dma((SLOTS,)), dma((2, 4))],
        compiler_params=pltpu.CompilerParams(collective_id=0, has_side_effects=True),
        cost_estimate=pl.CostEstimate(flops=2 ** 34, bytes_accessed=2 ** 26, transcendentals=0),
        name='front',
    )(residual, ln_scale[None, :], w_query, w_key, w_value, w_gate, w_up)


def own_kernel(hn_ref, wg_ref, wu_ref, out_ref):
    step = pl.program_id(0)
    half = pl.num_programs(0) // 2

    @pl.when(step < half)
    def _():
        out_ref[...] = jnp.dot(hn_ref[...], wg_ref[...], preferred_element_type=F32).astype(BF16)

    @pl.when(step >= half)
    def _():
        out_ref[...] = jnp.dot(hn_ref[...], wu_ref[...], preferred_element_type=F32).astype(BF16)


def own_gate_up(hn, w_gate, w_up):
    rows, depth = hn.shape
    ff = w_gate.shape[1]
    per = ff // WCOLS
    return pl.pallas_call(
        own_kernel,
        grid=(2 * per,),
        out_shape=jax.ShapeDtypeStruct((rows, 2 * ff), BF16),
        in_specs=[pl.BlockSpec((rows, depth), lambda i: (0, 0)),
                  pl.BlockSpec((depth, WCOLS), lambda i: (0, jnp.minimum(i, per - 1))),
                  pl.BlockSpec((depth, WCOLS), lambda i: (0, jnp.maximum(i - per, 0)))],
        out_specs=pl.BlockSpec((rows, WCOLS), lambda i: (0, i)),
        cost_estimate=pl.CostEstimate(flops=2 ** 33, bytes_accessed=2 ** 25, transcendentals=0),
        name='own_gate_up',
    )(hn, w_gate, w_up)


def attend_kernel(len_ref, q_ref, knew_ref, vnew_ref, kc_ref, vc_ref, o_ref, kout_ref, vout_ref):
    step = pl.program_id(0)
    rows = q_ref.shape[0]
    seq = kc_ref.shape[1]
    scale = q_ref.shape[2] ** -0.5
    for row in range(rows):
        pos = len_ref[step * rows + row]
        start = pl.multiple_of((pos // 16) * 16, 16)
        hit = lax.broadcasted_iota(jnp.int32, (16, 1), 0) == pos - start
        for cache, new, out in ((kc_ref, knew_ref, kout_ref), (vc_ref, vnew_ref, vout_ref)):
            out[row] = cache[row]
            window = cache[row, pl.ds(start, 16), :].astype(F32)
            out[row, pl.ds(start, 16), :] = jnp.where(hit, new[row].astype(F32), window).astype(BF16)
    for row in range(rows):
        pos = len_ref[step * rows + row]
        scores = lax.dot_general(q_ref[row], kout_ref[row], (((1,), (1,)), ((), ())), preferred_element_type=F32) * scale
        where = lax.broadcasted_iota(jnp.int32, (1, seq), 1) <= pos
        scores = jnp.where(where, scores, -1e30)
        top = jnp.max(scores, axis=1, keepdims=True)
        weight = jnp.exp(scores - top)
        probs = (weight / jnp.sum(weight, axis=1, keepdims=True)).astype(BF16)
        o_ref[row] = jnp.dot(probs, vout_ref[row], preferred_element_type=F32).astype(BF16)


def attend(lengths, query, key_new, value_new, k_cache, v_cache):
    rows, heads, dim = query.shape
    seq = k_cache.shape[1]
    small = pl.BlockSpec((ATTN_ROWS, heads, dim), lambda i, lens: (i, 0, 0))
    new = pl.BlockSpec((ATTN_ROWS, 1, dim), lambda i, lens: (i, 0, 0))
    big = pl.BlockSpec((ATTN_ROWS, seq, dim), lambda i, lens: (i, 0, 0))
    return pl.pallas_call(
        attend_kernel,
        grid_spec=pltpu.PrefetchScalarGridSpec(
            num_scalar_prefetch=1, grid=(rows // ATTN_ROWS,),
            in_specs=[small, new, new, big, big], out_specs=[small, big, big]),
        out_shape=(jax.ShapeDtypeStruct(query.shape, BF16),
                   jax.ShapeDtypeStruct(k_cache.shape, BF16),
                   jax.ShapeDtypeStruct(v_cache.shape, BF16)),
        compiler_params=pltpu.CompilerParams(vmem_limit_bytes=40 * 2 ** 20),
        cost_estimate=pl.CostEstimate(flops=2 ** 33, bytes_accessed=2 ** 27, transcendentals=2 ** 20),
        name='attend',
    )(lengths, query, key_new[:, None, :], value_new[:, None, :], k_cache, v_cache)


def scatter_kernel(part_ref, res_ref, out_ref, recv, send_sem, recv_sem):
    ty = lax.axis_index('tyz')
    width = out_ref.shape[1]
    barrier = pltpu.get_barrier_semaphore()
    for off in range(1, 4):
        pl.semaphore_signal(barrier, inc=1, device_id={'tyz': lax.rem(ty + off, 4)}, device_id_type=MESH)
    pl.semaphore_wait(barrier, 3)
    copies = []
    for off in (2, 1, 3):
        peer = lax.rem(ty + off, 4)
        copy = pltpu.make_async_remote_copy(
            part_ref.at[:, pl.ds(pl.multiple_of(peer * width, width), width)], recv.at[off],
            send_sem.at[off], recv_sem.at[off], device_id={'tyz': peer}, device_id_type=MESH)
        copy.start()
        copies.append(copy)
    total = part_ref[:, pl.ds(pl.multiple_of(ty * width, width), width)].astype(F32)
    for copy in copies:
        copy.wait()
    for off in range(1, 4):
        total = total + recv[off].astype(F32)
    out_ref[...] = (res_ref[...].astype(F32) + total).astype(out_ref.dtype)


def scatter_sum(part, residual):
    dma = pltpu.SemaphoreType.DMA
    vmem = pl.BlockSpec(memory_space=pltpu.VMEM)
    return pl.pallas_call(
        scatter_kernel,
        out_shape=jax.ShapeDtypeStruct(residual.shape, residual.dtype),
        in_specs=[vmem] * 2,
        out_specs=vmem,
        scratch_shapes=[pltpu.VMEM((4,) + residual.shape, BF16), dma((4,)), dma((4,))],
        compiler_params=pltpu.CompilerParams(collective_id=1, has_side_effects=True),
        cost_estimate=pl.CostEstimate(flops=2 ** 30, bytes_accessed=2 ** 22, transcendentals=0),
        name='scatter_sum',
    )(part, residual)


def solution(mesh):
    tx_size = mesh.shape['tx']
    tyz_size = mesh.shape['tyz']
    row_axes = ('dp', 'tx', 'tyz')
    swap = [(0, 1), (1, 0)]

    def rotate(vectors, cos_part, sin_part):
        half = vectors.shape[-1] // 2
        first = vectors[..., :half].astype(F32)
        second = vectors[..., half:].astype(F32)
        return jnp.concatenate([first * cos_part - second * sin_part, second * cos_part + first * sin_part], axis=-1).astype(BF16)

    def decode_layer(residual, ln_scale, w_query, w_key, w_value, w_gate, w_up, w_out, w_down, k_cache, v_cache, lengths):
        tx = lax.axis_index('tx')
        ty = lax.axis_index('tyz')
        rows, width = residual.shape
        half = rows // tx_size
        rows_local = k_cache.shape[0]
        head_dim = w_key.shape[1]

        def dot(a, b):
            return jnp.dot(a, b, preferred_element_type=F32)

        def pass_on(x):
            return lax.ppermute(x, 'tx', swap)

        *gate_up, mine, query_rows, key_new, value_new = front(residual, ln_scale, w_query, w_key, w_value, w_gate, w_up, rows_local)
        gate_up_got = [pass_on(x) for x in gate_up]
        gate_up_mine = own_gate_up(mine, w_gate, w_up)
        blocks = len(gate_up)
        size = half // blocks
        ff = w_gate.shape[1]

        half_dim = head_dim // 2
        inv_freq = ROPE_BASE ** (-2.0 * jnp.arange(half_dim, dtype=F32) / head_dim)
        angles = lengths.astype(F32)[:, None] * inv_freq[None, :]
        cos_part = jnp.cos(angles)
        sin_part = jnp.sin(angles)
        query_mine = lax.all_to_all(query_rows.reshape(half, -1, head_dim), 'tyz', 0, 1, tiled=True)
        query_rot = rotate(query_mine, cos_part[:, None], sin_part[:, None])
        key_rot = rotate(key_new, cos_part, sin_part)
        query_rot, gate_up_mine = lax.optimization_barrier((query_rot, gate_up_mine))
        attended, k_updated, v_updated = attend(lengths, query_rot, key_rot, value_new, k_cache, v_cache)
        attended_mine = lax.all_to_all(attended, 'tyz', 1, 0, tiled=True).reshape(half, -1)
        attended_other = pass_on(attended_mine)

        acts = []
        acts_got = []
        for idx in range(blocks):
            both = gate_up_mine[idx * size:(idx + 1) * size].astype(F32) + gate_up_got[idx].astype(F32)
            both = both.astype(BF16).astype(F32)
            gate, up = both[:, :ff], both[:, ff:]
            act = (jax.nn.silu(gate) * up).astype(BF16)
            acts.append(act)
            acts_got.append(pass_on(act))
        part_mine = dot(attended_mine, w_out) + dot(jnp.concatenate(acts, axis=0), w_down)
        res_mine = lax.dynamic_slice_in_dim(residual, tx * half, half, axis=0)
        res_other = lax.dynamic_slice_in_dim(residual, (1 - tx) * half, half, axis=0)
        out_mine = scatter_sum(part_mine.astype(BF16), res_mine)
        part_other = dot(attended_other, w_out) + dot(jnp.concatenate(acts_got, axis=0), w_down)
        out_other = scatter_sum(part_other.astype(BF16), res_other)
        new_resid = jnp.where(tx == 0, jnp.concatenate([out_mine, out_other]), jnp.concatenate([out_other, out_mine]))
        return new_resid, k_updated, v_updated

    in_specs = (P('dp', ('tx', 'tyz')), P(('tx', 'tyz')), P('tx', 'tyz'), P('tx', None), P('tx', None), P('tx', 'tyz'), P('tx', 'tyz'), P('tyz', 'tx'), P('tyz', 'tx'), P(row_axes, None, None), P(row_axes, None, None), P(row_axes))
    out_specs = (P('dp', ('tx', 'tyz')), P(row_axes, None, None), P(row_axes, None, None))
    return jax.shard_map(decode_layer, mesh=mesh, in_specs=in_specs, out_specs=out_specs, check_vma=False)
```

```python
import functools

import jax
import jax.numpy as jnp
from jax import lax
from jax.experimental import pallas as pl
from jax.experimental.pallas import tpu as pltpu
from jax.sharding import PartitionSpec as P

LN_EPS = 1e-5
ROPE_BASE = 10000.0
MESH = pl.DeviceIdType.MESH
F32 = jnp.float32
BF16 = jnp.bfloat16
CHUNKS = 4
SLOTS = 4
WCOLS = 512
EARLY = 12
ATTN_ROWS = 4


def front_kernel(res_ref, ln_ref, wq_ref, wk_ref, wv_ref, wg_ref, wu_ref,
                 got_ref, gu0_ref, gu1_ref, gu2_ref, gu3_ref, mine_ref, q_ref, k_ref, v_ref,
                 raw, hn, wq, wkv, slots, stage, first, stat, stats, lnb, lns, colstat, q_send, q_got, q_own, kv_send, kv_got,
                 stat_send, stat_recv, ln_send, ln_recv, pair_send, pair_recv, x_send, x_recv, relay_send, relay_recv,
                 q_ssem, q_rsem, kv_ssem, kv_rsem, wq_sem, slot_sem, out_sem, first_ssem, first_rsem, a2a_ssem, a2a_rsem):
    tx = lax.axis_index('tx')
    ty = lax.axis_index('tyz')
    rows, width = res_ref.shape
    half = rows // 2
    model_dim = 8 * width
    chunk = rows // CHUNKS
    pair = ty + 1 - 2 * lax.rem(ty, 2)
    across = lax.rem(ty + 2, 4)
    me = tx * 4 + ty
    few = k_ref.shape[0]
    dim = k_ref.shape[1]
    wcols = slots.shape[2]
    ff = wg_ref.shape[1]
    per = ff // wcols

    def dot(a, b):
        return jnp.dot(a, b, preferred_element_type=F32)

    weights = [pltpu.make_async_copy(wq_ref, wq, wq_sem.at[0]),
               pltpu.make_async_copy(wk_ref, wkv.at[:, pl.ds(0, dim)], wq_sem.at[1]),
               pltpu.make_async_copy(wv_ref, wkv.at[:, pl.ds(dim, dim)], wq_sem.at[2])]
    for copy in weights:
        copy.start()

    def fetch(ref, idx, slot):
        start = pl.multiple_of(idx * wcols, wcols)
        return pltpu.make_async_copy(ref.at[:, pl.ds(start, wcols)], slots.at[slot], slot_sem.at[slot])

    for idx in range(SLOTS - 1):
        fetch(wg_ref, idx, idx).start()

    barrier = pltpu.get_barrier_semaphore()
    for off in range(1, 8):
        peer = lax.rem(me + off, 8)
        pl.semaphore_signal(barrier, inc=1, device_id={'tx': peer // 4, 'tyz': lax.rem(peer, 4)}, device_id_type=MESH)
    lnb[...] = jnp.broadcast_to(ln_ref[...].astype(F32)[None, :], lnb.shape).astype(BF16)
    pl.semaphore_wait(barrier, 7)

    def cols(who):
        return pl.ds(pl.multiple_of(who * width, width), width)

    def actual(idx):
        start = (1 - tx) * half + idx * chunk if idx < CHUNKS // 2 else tx * half + idx * chunk - half
        return pl.ds(pl.multiple_of(start, chunk), chunk)

    def block(idx):
        return pl.ds(idx * chunk, chunk)

    copies = []
    crossing = []
    paired = []
    relayed = []
    for idx in range(CHUNKS):
        crossing.append(pltpu.make_async_remote_copy(
            res_ref.at[actual(idx)], raw.at[block(idx), cols(ty)], x_send.at[idx], x_recv.at[idx],
            device_id={'tyz': across}, device_id_type=MESH))
        paired.append(pltpu.make_async_remote_copy(
            res_ref.at[actual(idx)], raw.at[block(idx), cols(ty)], pair_send.at[idx], pair_recv.at[idx],
            device_id={'tyz': pair}, device_id_type=MESH))
        relayed.append(pltpu.make_async_remote_copy(
            raw.at[block(idx), cols(across)], raw.at[block(idx), cols(across)], relay_send.at[idx], relay_recv.at[idx],
            device_id={'tyz': pair}, device_id_type=MESH))
    crossing[0].start()
    paired[0].start()

    res = res_ref[...].astype(F32)
    row_sum = jnp.sum(res, axis=1, keepdims=True)
    row_sq = jnp.sum(jnp.square(res - row_sum / width), axis=1, keepdims=True)
    lane = lax.broadcasted_iota(jnp.int32, (rows, 128), 1)
    both = jnp.where(lax.rem(lane, 8) < 4, row_sum, row_sq)
    stat[...] = both.T[:8]
    for idx in range(CHUNKS):
        raw[block(idx), cols(ty)] = res_ref[actual(idx), :]
    lns[:, cols(ty)] = lnb[...]
    stats[me] = stat[...]
    for off in range(1, 8):
        peer = lax.rem(me + off, 8)
        copies.append(pltpu.make_async_remote_copy(
            stat, stats.at[me], stat_send.at[off], stat_recv.at[off],
            device_id={'tx': peer // 4, 'tyz': lax.rem(peer, 4)}, device_id_type=MESH))
    for off in range(1, 4):
        copies.append(pltpu.make_async_remote_copy(
            lnb, lns.at[:, cols(ty)], ln_send.at[off], ln_recv.at[off],
            device_id={'tyz': lax.rem(ty + off, 4)}, device_id_type=MESH))
    for copy in copies:
        copy.start()
    for idx in range(1, CHUNKS):
        crossing[idx].start()
        paired[idx].start()
    for copy in copies:
        copy.wait_recv()
    total = stats[0][:1]
    for src in range(1, 8):
        total = total + stats[src][:1]
    mean = total / model_dim
    square = jnp.zeros_like(mean)
    for src in range(8):
        square = square + stats[src][4:5] + width * jnp.square(stats[src][:1] / width - mean)
    scale = lax.rsqrt(square / model_dim + LN_EPS)
    upper = lax.broadcasted_iota(jnp.int32, (128, rows), 0) < 64
    cstat = jnp.where(upper, mean, scale).T
    start_mine = pl.multiple_of(tx * half, half)
    start_other = pl.multiple_of((1 - tx) * half, half)
    colstat[...] = cstat

    def norm(idx):
        centre = colstat[actual(idx), :][:, :1]
        factor = colstat[actual(idx), :][:, 64:65]
        for col in range(4):
            part = pl.ds(col * width, width)
            hn[block(idx), part] = ((raw[block(idx), part].astype(F32) - centre) * factor
                                    * lns[:1, part].astype(F32)).astype(BF16)

    q_copies = []
    for idx in range(CHUNKS // 2):
        crossing[idx].wait_recv()
        relayed[idx].start()
        paired[idx].wait_recv()
        relayed[idx].wait_recv()
        norm(idx)
        if idx == 0:
            weights[0].wait()
        q_send[block(idx), :] = dot(hn[block(idx), :], wq[...]).astype(BF16)
        copy = pltpu.make_async_remote_copy(
            q_send.at[block(idx)], q_got.at[block(idx)], q_ssem.at[idx], q_rsem.at[idx],
            device_id={'tx': 1 - tx}, device_id_type=MESH)
        copy.start()
        q_copies.append(copy)
    weights[1].wait()
    weights[2].wait()
    mine_few = pl.ds(pl.multiple_of(ty * few, few), few)
    kv_send[...] = dot(hn[mine_few, :], wkv[...]).astype(BF16)
    kv_copy = pltpu.make_async_remote_copy(kv_send, kv_got, kv_ssem, kv_rsem, device_id={'tx': 1 - tx}, device_id_type=MESH)
    kv_copy.start()

    for idx in range(CHUNKS // 2, CHUNKS):
        crossing[idx].wait_recv()
        relayed[idx].start()
    for idx in range(CHUNKS // 2, CHUNKS):
        paired[idx].wait_recv()
        relayed[idx].wait_recv()
        norm(idx)

    outs = (gu1_ref, gu2_ref, gu3_ref)
    size = half // (len(outs) + 1)

    def columns(step):
        return pl.ds(pl.multiple_of(step * wcols, wcols), wcols)

    def put(step, slot):
        out = [pltpu.make_async_copy(stage.at[slot, pl.ds((idx + 1) * size, size)], out.at[:, columns(step)], out_sem.at[slot, idx])
               for idx, out in enumerate(outs)]
        out.append(pltpu.make_async_copy(stage.at[slot, pl.ds(half, half)], mine_ref.at[:, columns(step)], out_sem.at[slot, 3]))
        return out

    def put_rest(step, slot):
        return pltpu.make_async_copy(stage.at[slot, pl.ds(0, size)], gu0_ref.at[:, columns(step - EARLY)], out_sem.at[slot, 4])

    def send_first(step):
        return pltpu.make_async_remote_copy(
            first.at[:, columns(step)], got_ref.at[:, columns(step)], first_ssem.at[step], first_rsem.at[step],
            device_id={'tx': 1 - tx}, device_id_type=MESH)

    def body(step, carry, gate):
        slot = lax.rem(step, SLOTS)
        side = lax.rem(step, 2)
        ahead = step + SLOTS - 1
        into = lax.rem(ahead, SLOTS)
        if gate:
            @pl.when(ahead < per)
            def _():
                fetch(wg_ref, ahead, into).start()

            @pl.when(ahead >= per)
            def _():
                fetch(wu_ref, ahead - per, into).start()
            fetch(wg_ref, 0, slot).wait()
        else:
            @pl.when(ahead < 2 * per)
            def _():
                fetch(wu_ref, ahead - per, into).start()
            fetch(wu_ref, 0, slot).wait()

        @pl.when(step >= 2)
        def _():
            for copy in put(step - 2, side):
                copy.wait()
        if not gate:
            @pl.when(step >= EARLY + 2)
            def _():
                put_rest(step - 2, side).wait()
        stage[side] = dot(hn[...], slots[slot]).astype(BF16)
        for copy in put(step, side):
            copy.start()
        if gate:
            first[:, columns(step)] = stage[side, :size, :]
            send_first(step).start()
        else:
            @pl.when(step < EARLY)
            def _():
                first[:, columns(step)] = stage[side, :size, :]
                send_first(step).start()

            @pl.when(step >= EARLY)
            def _():
                put_rest(step, side).start()
        return carry

    lax.fori_loop(0, per, functools.partial(body, gate=True), 0)
    q_own[...] = dot(hn[half:, :], wq[...]).astype(BF16)
    own_few = pl.ds(pl.multiple_of(half + ty * few, few), few)
    kv_own = dot(hn[own_few, :], wkv[...])
    kv_copy.wait()
    kv = (kv_own + kv_got[...].astype(F32)).astype(BF16)
    k_ref[...] = kv[:, :dim]
    v_ref[...] = kv[:, dim:]
    for copy in q_copies:
        copy.wait()
    q_own[...] = (q_own[...].astype(F32) + q_got[...].astype(F32)).astype(BF16)
    q_ref[ty] = q_own[mine_few, :]
    spread = []
    for off in (2, 1, 3):
        peer = lax.rem(ty + off, 4)
        spread.append(pltpu.make_async_remote_copy(
            q_own.at[pl.ds(pl.multiple_of(peer * few, few), few)], q_ref.at[ty], a2a_ssem.at[off], a2a_rsem.at[off],
            device_id={'tyz': peer}, device_id_type=MESH))
    for copy in spread:
        copy.start()
    lax.fori_loop(per, 2 * per, functools.partial(body, gate=False), 0)
    for copy in spread:
        copy.wait()
    for copy in copies + crossing + paired + relayed:
        copy.wait_send()
    for step in (2 * per - 2, 2 * per - 1):
        for copy in put(step, step % 2):
            copy.wait()
        put_rest(step, step % 2).wait()
    for step in range(EARLY):
        send_first(step).wait()


def front(residual, ln_scale, w_query, w_key, w_value, w_gate, w_up, few):
    rows, width = residual.shape
    half = rows // 2
    depth, q_cols = w_query.shape
    dim = w_key.shape[1]
    ff = w_gate.shape[1]
    dma = pltpu.SemaphoreType.DMA
    vmem = pl.BlockSpec(memory_space=pltpu.VMEM)
    hbm = pl.BlockSpec(memory_space=pl.ANY)
    shape = jax.ShapeDtypeStruct
    size = half // 4
    return pl.pallas_call(
        front_kernel,
        out_shape=(shape((size, EARLY * WCOLS), BF16), shape((size, 2 * ff - EARLY * WCOLS), BF16)) + (shape((size, 2 * ff), BF16),) * 3
        + (shape((half, 2 * ff), BF16), shape((4, few, q_cols), BF16), shape((few, dim), BF16), shape((few, dim), BF16)),
        in_specs=[vmem] * 2 + [hbm] * 5,
        out_specs=(hbm,) * 6 + (vmem,) * 3,
        scratch_shapes=[
            pltpu.VMEM((rows, depth), BF16), pltpu.VMEM((rows, depth), BF16),
            pltpu.VMEM((depth, q_cols), BF16), pltpu.VMEM((depth, 2 * dim), BF16),
            pltpu.VMEM((SLOTS, depth, WCOLS), BF16), pltpu.VMEM((2, rows, WCOLS), BF16), pltpu.VMEM((size, EARLY * WCOLS), BF16),
            pltpu.VMEM((8, rows), F32), pltpu.VMEM((8, 8, rows), F32),
            pltpu.VMEM((16, width), BF16), pltpu.VMEM((16, depth), BF16), pltpu.VMEM((rows, 128), F32),
            pltpu.VMEM((half, q_cols), BF16), pltpu.VMEM((half, q_cols), BF16), pltpu.VMEM((half, q_cols), BF16),
            pltpu.VMEM((few, 2 * dim), BF16), pltpu.VMEM((few, 2 * dim), BF16),
            dma((8,)), dma((8,)), dma((4,)), dma((4,)), dma((CHUNKS,)), dma((CHUNKS,)), dma((CHUNKS,)), dma((CHUNKS,)),
            dma((CHUNKS,)), dma((CHUNKS,)), dma((CHUNKS,)), dma((CHUNKS,)), dma, dma, dma((3,)), dma((SLOTS,)), dma((2, 5)),
            dma((EARLY,)), dma((EARLY,)), dma((4,)), dma((4,))],
        compiler_params=pltpu.CompilerParams(collective_id=0, has_side_effects=True),
        cost_estimate=pl.CostEstimate(flops=2 ** 34, bytes_accessed=2 ** 26, transcendentals=0),
        name='front',
    )(residual, ln_scale, w_query, w_key, w_value, w_gate, w_up)


def attend_kernel(len_ref, q_ref, knew_ref, vnew_ref, kc_ref, vc_ref, o_ref, kout_ref, vout_ref):
    step = pl.program_id(0)
    rows = q_ref.shape[0]
    seq = kc_ref.shape[1]
    scale = q_ref.shape[2] ** -0.5
    for row in range(rows):
        pos = len_ref[step * rows + row]
        start = pl.multiple_of((pos // 16) * 16, 16)
        hit = lax.broadcasted_iota(jnp.int32, (16, 1), 0) == pos - start
        for cache, new, out in ((kc_ref, knew_ref, kout_ref), (vc_ref, vnew_ref, vout_ref)):
            out[row] = cache[row]
            window = cache[row, pl.ds(start, 16), :].astype(F32)
            out[row, pl.ds(start, 16), :] = jnp.where(hit, new[row].astype(F32), window).astype(BF16)
    for row in range(rows):
        pos = len_ref[step * rows + row]
        scores = lax.dot_general(q_ref[row], kout_ref[row], (((1,), (1,)), ((), ())), preferred_element_type=F32) * scale
        where = lax.broadcasted_iota(jnp.int32, (1, seq), 1) <= pos
        scores = jnp.where(where, scores, -1e30)
        top = jnp.max(scores, axis=1, keepdims=True)
        weight = jnp.exp(scores - top)
        probs = (weight / jnp.sum(weight, axis=1, keepdims=True)).astype(BF16)
        o_ref[row] = jnp.dot(probs, vout_ref[row], preferred_element_type=F32).astype(BF16)


def attend(lengths, query, key_new, value_new, k_cache, v_cache):
    rows, heads, dim = query.shape
    seq = k_cache.shape[1]
    small = pl.BlockSpec((ATTN_ROWS, heads, dim), lambda i, lens: (i, 0, 0))
    new = pl.BlockSpec((ATTN_ROWS, 1, dim), lambda i, lens: (i, 0, 0))
    big = pl.BlockSpec((ATTN_ROWS, seq, dim), lambda i, lens: (i, 0, 0))
    return pl.pallas_call(
        attend_kernel,
        grid_spec=pltpu.PrefetchScalarGridSpec(
            num_scalar_prefetch=1, grid=(rows // ATTN_ROWS,),
            in_specs=[small, new, new, big, big], out_specs=[small, big, big]),
        out_shape=(jax.ShapeDtypeStruct(query.shape, BF16),
                   jax.ShapeDtypeStruct(k_cache.shape, BF16),
                   jax.ShapeDtypeStruct(v_cache.shape, BF16)),
        compiler_params=pltpu.CompilerParams(vmem_limit_bytes=40 * 2 ** 20),
        cost_estimate=pl.CostEstimate(flops=2 ** 33, bytes_accessed=2 ** 27, transcendentals=2 ** 20),
        name='attend',
    )(lengths, query, key_new[:, None, :], value_new[:, None, :], k_cache, v_cache)


def scatter_kernel(part_ref, res_ref, out_ref, recv, send_sem, recv_sem):
    ty = lax.axis_index('tyz')
    width = out_ref.shape[1]
    barrier = pltpu.get_barrier_semaphore()
    for off in range(1, 4):
        pl.semaphore_signal(barrier, inc=1, device_id={'tyz': lax.rem(ty + off, 4)}, device_id_type=MESH)
    pl.semaphore_wait(barrier, 3)
    copies = []
    for off in (2, 1, 3):
        peer = lax.rem(ty + off, 4)
        copy = pltpu.make_async_remote_copy(
            part_ref.at[:, pl.ds(pl.multiple_of(peer * width, width), width)], recv.at[off],
            send_sem.at[off], recv_sem.at[off], device_id={'tyz': peer}, device_id_type=MESH)
        copy.start()
        copies.append(copy)
    total = part_ref[:, pl.ds(pl.multiple_of(ty * width, width), width)].astype(F32)
    for copy in copies:
        copy.wait()
    for off in range(1, 4):
        total = total + recv[off].astype(F32)
    out_ref[...] = (res_ref[...].astype(F32) + total).astype(out_ref.dtype)


def scatter_sum(part, residual):
    dma = pltpu.SemaphoreType.DMA
    vmem = pl.BlockSpec(memory_space=pltpu.VMEM)
    return pl.pallas_call(
        scatter_kernel,
        out_shape=jax.ShapeDtypeStruct(residual.shape, residual.dtype),
        in_specs=[vmem] * 2,
        out_specs=vmem,
        scratch_shapes=[pltpu.VMEM((4,) + residual.shape, BF16), dma((4,)), dma((4,))],
        compiler_params=pltpu.CompilerParams(collective_id=1, has_side_effects=True),
        cost_estimate=pl.CostEstimate(flops=2 ** 30, bytes_accessed=2 ** 22, transcendentals=0),
        name='scatter_sum',
    )(part, residual)


def solution(mesh):
    tx_size = mesh.shape['tx']
    tyz_size = mesh.shape['tyz']
    row_axes = ('dp', 'tx', 'tyz')
    swap = [(0, 1), (1, 0)]

    def rotate(vectors, cos_part, sin_part):
        half = vectors.shape[-1] // 2
        first = vectors[..., :half].astype(F32)
        second = vectors[..., half:].astype(F32)
        return jnp.concatenate([first * cos_part - second * sin_part, second * cos_part + first * sin_part], axis=-1).astype(BF16)

    def decode_layer(residual, ln_scale, w_query, w_key, w_value, w_gate, w_up, w_out, w_down, k_cache, v_cache, lengths):
        tx = lax.axis_index('tx')
        ty = lax.axis_index('tyz')
        rows, width = residual.shape
        half = rows // tx_size
        rows_local = k_cache.shape[0]
        head_dim = w_key.shape[1]

        def dot(a, b):
            return jnp.dot(a, b, preferred_element_type=F32)

        def pass_on(x):
            return lax.ppermute(x, 'tx', swap)

        got, *gate_up, gate_up_mine, query_mine, key_new, value_new = front(residual, ln_scale, w_query, w_key, w_value, w_gate, w_up, rows_local)
        gate_up_got = [pass_on(x) for x in gate_up]
        gate_up_got[0] = jnp.concatenate([got, gate_up_got[0]], axis=1)
        blocks = len(gate_up)
        size = half // blocks
        ff = w_gate.shape[1]

        half_dim = head_dim // 2
        inv_freq = ROPE_BASE ** (-2.0 * jnp.arange(half_dim, dtype=F32) / head_dim)
        angles = lengths.astype(F32)[:, None] * inv_freq[None, :]
        cos_part = jnp.cos(angles)
        sin_part = jnp.sin(angles)
        query_mine = query_mine.reshape(4, rows_local, -1, head_dim).transpose(1, 0, 2, 3).reshape(rows_local, -1, head_dim)
        query_rot = rotate(query_mine, cos_part[:, None], sin_part[:, None])
        key_rot = rotate(key_new, cos_part, sin_part)
        attended, k_updated, v_updated = attend(lengths, query_rot, key_rot, value_new, k_cache, v_cache)
        attended_mine = lax.all_to_all(attended, 'tyz', 1, 0, tiled=True).reshape(half, -1)
        attended_other = pass_on(attended_mine)

        acts = []
        acts_got = []
        for idx in range(blocks):
            both = gate_up_mine[idx * size:(idx + 1) * size].astype(F32) + gate_up_got[idx].astype(F32)
            both = both.astype(BF16).astype(F32)
            gate, up = both[:, :ff], both[:, ff:]
            act = (jax.nn.silu(gate) * up).astype(BF16)
            acts.append(act)
            acts_got.append(pass_on(act))
        part_mine = dot(attended_mine, w_out) + dot(jnp.concatenate(acts, axis=0), w_down)
        res_mine = lax.dynamic_slice_in_dim(residual, tx * half, half, axis=0)
        res_other = lax.dynamic_slice_in_dim(residual, (1 - tx) * half, half, axis=0)
        out_mine = scatter_sum(part_mine.astype(BF16), res_mine)
        part_other = dot(attended_other, w_out) + dot(jnp.concatenate(acts_got, axis=0), w_down)
        out_other = scatter_sum(part_other.astype(BF16), res_other)
        new_resid = jnp.where(tx == 0, jnp.concatenate([out_mine, out_other]), jnp.concatenate([out_other, out_mine]))
        return new_resid, k_updated, v_updated

    in_specs = (P('dp', ('tx', 'tyz')), P(('tx', 'tyz')), P('tx', 'tyz'), P('tx', None), P('tx', None), P('tx', 'tyz'), P('tx', 'tyz'), P('tyz', 'tx'), P('tyz', 'tx'), P(row_axes, None, None), P(row_axes, None, None), P(row_axes))
    out_specs = (P('dp', ('tx', 'tyz')), P(row_axes, None, None), P(row_axes, None, None))
    return jax.shard_map(decode_layer, mesh=mesh, in_specs=in_specs, out_specs=out_specs, check_vma=False)
```

```python
import functools

import jax
import jax.numpy as jnp
import numpy as np
from jax import lax
from jax.experimental import pallas as pl
from jax.experimental.pallas import tpu as pltpu
from jax.sharding import PartitionSpec as P


LN_EPS = 1e-5
ROPE_BASE = 10000.0
MESH = pl.DeviceIdType.MESH
F32 = jnp.float32
BF16 = jnp.bfloat16
SPANS = ((0, 32), (32, 64), (96, 64), (160, 96), (256, 128), (384, 128))
CHUNKS = len(SPANS)
EARLY = 4
SLOTS = 4
WCOLS = 512
SIZES = (80, 80, 64, 32)
STARTS = (0, 80, 160, 224)
PIECES = (2, 4, 4, 4)
HBM = pl.BlockSpec(memory_space=pl.ANY)
ATTN_ROWS = 8


def front_kernel(res_in, ln_in, wq_ref, wk_ref, wv_ref, wg_ref, wu_ref,
                 got_ref, gu1_ref, gu2_ref, gu3_ref, mine0_ref, mine1_ref, mine2_ref, mine3_ref, q_ref, k_ref, v_ref,
                 res_ref, ln_ref, kv_new, raw, hn, wq, wkv, slots, stage, first, stat, stats, lnb, lns, colstat, q_send, q_got, q_own, kv_send, kv_got,
                 stat_send, stat_recv, ln_send, ln_recv, pair_send, pair_recv, x_send, x_recv, relay_send, relay_recv,
                 q_ssem, q_rsem, kv_ssem, kv_rsem, wq_sem, slot_sem, out_sem, first_ssem, first_rsem, a2a_ssem, a2a_rsem, in_sem, new_sem):
    tx = lax.axis_index('tx')
    ty = lax.axis_index('tyz')
    rows, width = res_ref.shape
    half = rows // 2
    model_dim = 8 * width
    pair = ty + 1 - 2 * lax.rem(ty, 2)
    across = lax.rem(ty + 2, 4)
    me = tx * 4 + ty
    few = k_ref.shape[0]
    dim = k_ref.shape[1]
    wcols = slots.shape[2]
    ff = wg_ref.shape[1]
    per = ff // wcols

    def dot(a, b):
        return jnp.dot(a, b, preferred_element_type=F32)

    inputs = [pltpu.make_async_copy(res_in, res_ref, in_sem.at[0]), pltpu.make_async_copy(ln_in, ln_ref, in_sem.at[1])]
    for copy in inputs:
        copy.start()
    weights = [pltpu.make_async_copy(wq_ref, wq, wq_sem.at[0]),
               pltpu.make_async_copy(wk_ref, wkv.at[:, pl.ds(0, dim)], wq_sem.at[1]),
               pltpu.make_async_copy(wv_ref, wkv.at[:, pl.ds(dim, dim)], wq_sem.at[2])]

    def fetch(ref, idx, slot):
        start = pl.multiple_of(idx * wcols, wcols)
        return pltpu.make_async_copy(ref.at[:, pl.ds(start, wcols)], slots.at[slot], slot_sem.at[slot])

    barrier = pltpu.get_barrier_semaphore()
    for off in range(1, 8):
        peer = lax.rem(me + off, 8)
        pl.semaphore_signal(barrier, inc=1, device_id={'tx': peer // 4, 'tyz': lax.rem(peer, 4)}, device_id_type=MESH)
    inputs[0].wait()
    for copy in weights:
        copy.start()
    for idx in range(SLOTS - 1):
        fetch(wg_ref, idx, idx).start()
    inputs[1].wait()
    lnb[...] = jnp.broadcast_to(ln_ref[...].astype(F32)[None, :], lnb.shape).astype(BF16)
    res = res_ref[...].astype(F32)
    row_sum = jnp.sum(res, axis=1, keepdims=True)
    row_sq = jnp.sum(jnp.square(res - row_sum / width), axis=1, keepdims=True)
    lane = lax.broadcasted_iota(jnp.int32, (rows, 128), 1)
    both = jnp.where(lax.rem(lane, 8) < 4, row_sum, row_sq).T[:8]
    sub = lax.rem(lax.broadcasted_iota(jnp.int32, (8, 128), 0), 4)
    packed = both[:, :128]
    for idx in range(1, rows // 128):
        packed = jnp.where(sub == idx, both[:, idx * 128:(idx + 1) * 128], packed)
    stat[...] = packed
    pl.semaphore_wait(barrier, 7)

    def cols(who):
        return pl.ds(pl.multiple_of(who * width, width), width)

    def actual(idx):
        start, size = SPANS[idx]
        start = (1 - tx) * half + start if start < half else tx * half + start - half
        return pl.ds(pl.multiple_of(start, 32), size)

    def block(idx):
        return pl.ds(*SPANS[idx])

    copies = []
    crossing = []
    paired = []
    relayed = []
    for idx in range(CHUNKS):
        crossing.append(pltpu.make_async_remote_copy(
            res_ref.at[actual(idx)], raw.at[block(idx), cols(ty)], x_send.at[idx], x_recv.at[idx],
            device_id={'tyz': across}, device_id_type=MESH))
        paired.append(pltpu.make_async_remote_copy(
            res_ref.at[actual(idx)], raw.at[block(idx), cols(ty)], pair_send.at[idx], pair_recv.at[idx],
            device_id={'tyz': pair}, device_id_type=MESH))
        relayed.append(pltpu.make_async_remote_copy(
            raw.at[block(idx), cols(across)], raw.at[block(idx), cols(across)], relay_send.at[idx], relay_recv.at[idx],
            device_id={'tyz': pair}, device_id_type=MESH))
    stats[me] = stat[...]
    for off in range(1, 8):
        peer = lax.rem(me + off, 8)
        copies.append(pltpu.make_async_remote_copy(
            stat, stats.at[me], stat_send.at[off], stat_recv.at[off],
            device_id={'tx': peer // 4, 'tyz': lax.rem(peer, 4)}, device_id_type=MESH))
    for off in range(1, 4):
        copies.append(pltpu.make_async_remote_copy(
            lnb, lns.at[:, cols(ty)], ln_send.at[off], ln_recv.at[off],
            device_id={'tyz': lax.rem(ty + off, 4)}, device_id_type=MESH))
    for copy in copies:
        copy.start()
    for idx in range(CHUNKS):
        crossing[idx].start()
        paired[idx].start()
    for idx in range(CHUNKS):
        raw[block(idx), cols(ty)] = res_ref[actual(idx), :]
    lns[:, cols(ty)] = lnb[...]
    for copy in copies:
        copy.wait_recv()
    total = stats[0][:4]
    for src in range(1, 8):
        total = total + stats[src][:4]
    mean = total / model_dim
    square = jnp.zeros_like(mean)
    for src in range(8):
        square = square + stats[src][4:] + width * jnp.square(stats[src][:4] / width - mean)
    scale = lax.rsqrt(square / model_dim + LN_EPS)
    upper = lax.broadcasted_iota(jnp.int32, (128, 128), 0) < 64
    for idx in range(rows // 128):
        colstat[idx * 128:(idx + 1) * 128, :] = jnp.where(upper, mean[idx:idx + 1], scale[idx:idx + 1]).T

    def norm(idx):
        centre = colstat[actual(idx), :][:, :1]
        factor = colstat[actual(idx), :][:, 64:65]
        for col in range(4):
            part = pl.ds(col * width, width)
            hn[block(idx), part] = ((raw[block(idx), part].astype(F32) - centre) * factor
                                    * lns[:1, part].astype(F32)).astype(BF16)

    q_copies = []
    for idx in range(EARLY):
        crossing[idx].wait_recv()
        relayed[idx].start()
        paired[idx].wait_recv()
        relayed[idx].wait_recv()
        norm(idx)
        if idx == 0:
            weights[0].wait()
        q_send[block(idx), :] = dot(hn[block(idx), :], wq[...]).astype(BF16)
        copy = pltpu.make_async_remote_copy(
            q_send.at[block(idx)], q_got.at[block(idx)], q_ssem.at[idx], q_rsem.at[idx],
            device_id={'tx': 1 - tx}, device_id_type=MESH)
        copy.start()
        q_copies.append(copy)
    weights[1].wait()
    weights[2].wait()
    mine_few = pl.ds(pl.multiple_of(ty * few, few), few)
    kv_send[...] = dot(hn[mine_few, :], wkv[...]).astype(BF16)
    kv_copy = pltpu.make_async_remote_copy(kv_send, kv_got, kv_ssem, kv_rsem, device_id={'tx': 1 - tx}, device_id_type=MESH)
    kv_copy.start()

    for idx in range(EARLY, CHUNKS):
        crossing[idx].wait_recv()
        relayed[idx].start()
    for idx in range(EARLY, CHUNKS):
        paired[idx].wait_recv()
        relayed[idx].wait_recv()
        norm(idx)

    outs = ((gu1_ref, STARTS[1]), (gu2_ref, STARTS[2]), (gu3_ref, STARTS[3]), (mine0_ref, half), (mine1_ref, half + STARTS[1]),
            (mine2_ref, half + STARTS[2]), (mine3_ref, half + STARTS[3]))

    def columns(step):
        return pl.ds(pl.multiple_of(step * wcols, wcols), wcols)

    def put(step, slot):
        return [pltpu.make_async_copy(stage.at[slot, pl.ds(start, out.shape[0])], out.at[:, columns(step)], out_sem.at[slot, idx])
                for idx, (out, start) in enumerate(outs)]

    def send_first(step):
        return pltpu.make_async_remote_copy(
            first.at[:, columns(step)], got_ref.at[:, columns(step)], first_ssem.at[step], first_rsem.at[step],
            device_id={'tx': 1 - tx}, device_id_type=MESH)

    def body(step, carry, gate):
        slot = lax.rem(step, SLOTS)
        side = lax.rem(step, 2)
        ahead = step + SLOTS - 1
        into = lax.rem(ahead, SLOTS)
        if gate:
            @pl.when(ahead < per)
            def _():
                fetch(wg_ref, ahead, into).start()

            @pl.when(ahead >= per)
            def _():
                fetch(wu_ref, ahead - per, into).start()

            fetch(wg_ref, 0, slot).wait()
        else:
            @pl.when(ahead < 2 * per)
            def _():
                fetch(wu_ref, ahead - per, into).start()

            fetch(wu_ref, 0, slot).wait()

        @pl.when(step >= 2)
        def _():
            for copy in put(step - 2, side):
                copy.wait()

        stage[side] = dot(hn[...], slots[slot]).astype(BF16)
        for copy in put(step, side):
            copy.start()
        first[:, columns(step)] = stage[side, :SIZES[0], :]
        send_first(step).start()
        return carry

    lax.fori_loop(0, per, functools.partial(body, gate=True), 0)
    q_own[...] = dot(hn[half:, :], wq[...]).astype(BF16)
    own_few = pl.ds(pl.multiple_of(half + ty * few, few), few)
    kv_own = dot(hn[own_few, :], wkv[...])
    kv_copy.wait()
    kv = (kv_own + kv_got[...].astype(F32)).astype(BF16)
    kv_new[0] = kv[:, :dim]
    kv_new[1] = kv[:, dim:]
    for copy in q_copies:
        copy.wait()
    q_own[...] = (q_own[...].astype(F32) + q_got[...].astype(F32)).astype(BF16)
    news = [pltpu.make_async_copy(kv_new.at[0], k_ref, new_sem.at[0]), pltpu.make_async_copy(kv_new.at[1], v_ref, new_sem.at[1]),
            pltpu.make_async_copy(q_own.at[mine_few], q_ref.at[ty], new_sem.at[2])]
    spread = []
    for off in (2, 1, 3):
        peer = lax.rem(ty + off, 4)
        spread.append(pltpu.make_async_remote_copy(
            q_own.at[pl.ds(pl.multiple_of(peer * few, few), few)], q_ref.at[ty], a2a_ssem.at[off], a2a_rsem.at[off],
            device_id={'tyz': peer}, device_id_type=MESH))
    for copy in spread + news:
        copy.start()
    lax.fori_loop(per, 2 * per, functools.partial(body, gate=False), 0)
    for copy in spread + news:
        copy.wait()
    for copy in copies + crossing + paired + relayed:
        copy.wait_send()
    for step in (2 * per - 2, 2 * per - 1):
        for copy in put(step, step % 2):
            copy.wait()
    for step in range(2 * per):
        send_first(step).wait()


def front(residual, ln_scale, w_query, w_key, w_value, w_gate, w_up, few):
    rows, width = residual.shape
    half = rows // 2
    depth, q_cols = w_query.shape
    dim = w_key.shape[1]
    ff = w_gate.shape[1]
    dma = pltpu.SemaphoreType.DMA
    shape = jax.ShapeDtypeStruct
    blocks = tuple(shape((size, 2 * ff), BF16) for size in SIZES)
    return pl.pallas_call(
        front_kernel,
        out_shape=blocks + blocks + (shape((4, few, q_cols), BF16), shape((few, dim), BF16), shape((few, dim), BF16)),
        in_specs=[HBM] * 7,
        out_specs=(HBM,) * 11,
        scratch_shapes=[
            pltpu.VMEM((rows, width), BF16), pltpu.VMEM((width,), BF16), pltpu.VMEM((2, few, dim), BF16),
            pltpu.VMEM((rows, depth), BF16), pltpu.VMEM((rows, depth), BF16),
            pltpu.VMEM((depth, q_cols), BF16), pltpu.VMEM((depth, 2 * dim), BF16),
            pltpu.VMEM((SLOTS, depth, WCOLS), BF16), pltpu.VMEM((2, rows, WCOLS), BF16), pltpu.VMEM((SIZES[0], 2 * ff), BF16),
            pltpu.VMEM((8, 128), F32), pltpu.VMEM((8, 8, 128), F32),
            pltpu.VMEM((16, width), BF16), pltpu.VMEM((16, depth), BF16), pltpu.VMEM((rows, 128), F32),
            pltpu.VMEM((half, q_cols), BF16), pltpu.VMEM((half, q_cols), BF16), pltpu.VMEM((half, q_cols), BF16),
            pltpu.VMEM((few, 2 * dim), BF16), pltpu.VMEM((few, 2 * dim), BF16),
            dma((8,)), dma((8,)), dma((4,)), dma((4,)), dma((CHUNKS,)), dma((CHUNKS,)), dma((CHUNKS,)), dma((CHUNKS,)),
            dma((CHUNKS,)), dma((CHUNKS,)), dma((CHUNKS,)), dma((CHUNKS,)), dma, dma, dma((3,)), dma((SLOTS,)), dma((2, 7)),
            dma((2 * ff // WCOLS,)), dma((2 * ff // WCOLS,)), dma((4,)), dma((4,)), dma((2,)), dma((3,))],
        compiler_params=pltpu.CompilerParams(collective_id=0, has_side_effects=True),
        cost_estimate=pl.CostEstimate(flops=2 ** 34, bytes_accessed=2 ** 26, transcendentals=0),
        name='front',
    )(residual, ln_scale, w_query, w_key, w_value, w_gate, w_up)


def attend_kernel(len_ref, freq_ref, q_ref, knew_ref, vnew_ref, kc_ref, vc_ref, o_ref, kout_ref, vout_ref, q_low, q_high, k_rot, v_new, o_low, o_high):
    step = pl.program_id(0)
    groups, rows, span = q_ref.shape
    seq, dim = kc_ref.shape[1:]
    heads = groups * span // dim
    half = dim // 2
    sub = lax.broadcasted_iota(jnp.int32, (rows, 1), 0)
    positions = jnp.zeros((rows, 1), jnp.int32)
    for row in range(rows):
        positions = jnp.where(sub == row, len_ref[step * rows + row], positions)
    angles = positions.astype(F32) * freq_ref[...]
    cos_part = jnp.cos(angles)
    sin_part = jnp.sin(angles)

    def rotate(first, second):
        first = first.astype(F32)
        second = second.astype(F32)
        return first * cos_part - second * sin_part, second * cos_part + first * sin_part

    k_rot[:, :half], k_rot[:, half:] = rotate(knew_ref[:, :half], knew_ref[:, half:])
    v_new[...] = vnew_ref[...].astype(F32)
    for head in range(heads):
        group, start = divmod(head * dim, span)
        place = pl.ds(head * rows, rows)
        q_low[place, :], q_high[place, :] = rotate(q_ref[group, :, start:start + half], q_ref[group, :, start + half:start + dim])
    for row in range(rows):
        pos = len_ref[step * rows + row]
        start = pl.multiple_of((pos // 16) * 16, 16)
        hit = lax.broadcasted_iota(jnp.int32, (16, 1), 0) == pos - start
        for cache, new, out in ((kc_ref, k_rot, kout_ref), (vc_ref, v_new, vout_ref)):
            out[row] = cache[row]
            window = cache[row, pl.ds(start, 16), :].astype(F32)
            out[row, pl.ds(start, 16), :] = jnp.where(hit, new[row:row + 1, :], window).astype(BF16)
    for row in range(rows):
        pos = len_ref[step * rows + row]
        place = pl.ds(row, heads, stride=rows)
        query = jnp.concatenate([q_low[place, :], q_high[place, :]], axis=1).astype(BF16)
        scores = lax.dot_general(query, kout_ref[row], (((1,), (1,)), ((), ())), preferred_element_type=F32) * dim ** -0.5
        where = lax.broadcasted_iota(jnp.int32, (1, seq), 1) <= pos
        scores = jnp.where(where, scores, -1e30)
        top = jnp.max(scores, axis=1, keepdims=True)
        weight = jnp.exp(scores - top)
        probs = (weight / jnp.sum(weight, axis=1, keepdims=True)).astype(BF16)
        total = jnp.dot(probs, vout_ref[row], preferred_element_type=F32)
        o_low[place, :] = total[:, :half]
        o_high[place, :] = total[:, half:]
    for head in range(heads):
        o_ref[:, head * dim:head * dim + half] = o_low[head * rows:(head + 1) * rows, :].astype(BF16)
        o_ref[:, head * dim + half:(head + 1) * dim] = o_high[head * rows:(head + 1) * rows, :].astype(BF16)


def attend(lengths, query, key_new, value_new, k_cache, v_cache):
    groups, rows, span = query.shape
    seq, dim = k_cache.shape[1:]
    width = groups * span
    freq = jnp.asarray(np.power(ROPE_BASE, -2.0 * np.arange(dim // 2) / dim)[None, :].astype(np.float32))
    new = pl.BlockSpec((ATTN_ROWS, dim), lambda i, lens: (i, 0))
    big = pl.BlockSpec((ATTN_ROWS, seq, dim), lambda i, lens: (i, 0, 0))
    return pl.pallas_call(
        attend_kernel,
        grid_spec=pltpu.PrefetchScalarGridSpec(
            num_scalar_prefetch=1, grid=(rows // ATTN_ROWS,),
            in_specs=[pl.BlockSpec((1, dim // 2), lambda i, lens: (0, 0)),
                      pl.BlockSpec((groups, ATTN_ROWS, span), lambda i, lens: (0, i, 0)), new, new, big, big],
            out_specs=[pl.BlockSpec((ATTN_ROWS, width), lambda i, lens: (i, 0)), big, big],
            scratch_shapes=[pltpu.VMEM((ATTN_ROWS * width // dim, dim // 2), F32)] * 2 + [pltpu.VMEM((ATTN_ROWS, dim), F32)] * 2
            + [pltpu.VMEM((ATTN_ROWS * width // dim, dim // 2), F32)] * 2),
        out_shape=(jax.ShapeDtypeStruct((rows, width), BF16),
                   jax.ShapeDtypeStruct(k_cache.shape, BF16),
                   jax.ShapeDtypeStruct(v_cache.shape, BF16)),
        compiler_params=pltpu.CompilerParams(vmem_limit_bytes=67043328),
        cost_estimate=pl.CostEstimate(flops=2 ** 33, bytes_accessed=2 ** 27, transcendentals=2 ** 20),
        name='attend',
    )(lengths, freq, query, key_new, value_new, k_cache, v_cache)


def tail_kernel(act0_ref, act1_ref, act2_ref, got_ref, mine_ref, att_in, wo_ref, wd_ref, res_in, out_ref,
                att_ref, res_ref, wo, wd, gu_got, gu_mine, act, act_got, o_mine, o_got, sums, out_buf,
                send_own, recv_own, keep_own, send0, recv0, keep0, send1, recv1, keep1, send2, recv2, keep2, send3, recv3, keep3,
                w_sem, gu_sem, o_ssem, o_rsem, a2a_ssem, a2a_rsem, act_ssem, act_rsem, own_ssem, own_rsem, row_ssem, row_rsem, out_sem):
    tx = lax.axis_index('tx')
    ty = lax.axis_index('tyz')
    few = att_ref.shape[0]
    half = 4 * few
    width = out_ref.shape[1]
    ff = act.shape[1]
    o_cols = o_mine.shape[1]
    acts = (act0_ref, act1_ref, act2_ref)

    def dot(a, b):
        return jnp.dot(a, b, preferred_element_type=F32)

    def peer_of(rel):
        return 2 * lax.rem(ty // 2 + rel // 2, 2) + lax.rem(lax.rem(ty, 2) + lax.rem(rel, 2), 2)

    weights = [pltpu.make_async_copy(wo_ref, wo, w_sem.at[0]), pltpu.make_async_copy(wd_ref, wd, w_sem.at[1]),
               pltpu.make_async_copy(res_in, res_ref, w_sem.at[2])]
    att_copy = pltpu.make_async_copy(att_in, att_ref, w_sem.at[3])
    loads = [pltpu.make_async_copy(mine_ref, gu_mine, gu_sem.at[3]), pltpu.make_async_copy(got_ref, gu_got, gu_sem.at[4])]
    held = [pltpu.make_async_copy(ref, act.at[pl.ds(STARTS[idx], SIZES[idx])], gu_sem.at[idx]) for idx, ref in enumerate(acts)]
    barrier = pltpu.get_barrier_semaphore()
    pl.semaphore_signal(barrier, inc=1, device_id={'tx': 1 - tx}, device_id_type=MESH)
    for rel in (1, 2, 3):
        pl.semaphore_signal(barrier, inc=1, device_id={'tyz': peer_of(rel)}, device_id_type=MESH)

    def silu(col, carry):
        part = pl.ds(pl.multiple_of(col * 512, 512), 512)
        other = pl.ds(pl.multiple_of(ff + col * 512, 512), 512)
        gate = (gu_mine[:, part].astype(F32) + gu_got[:, part].astype(F32)).astype(BF16).astype(F32)
        up = (gu_mine[:, other].astype(F32) + gu_got[:, other].astype(F32)).astype(BF16).astype(F32)
        act[STARTS[3]:, part] = (gate / (1.0 + jnp.exp(-gate)) * up).astype(BF16)
        return carry

    def act_copy(idx, where):
        piece = ff // PIECES[idx]
        sem = sum(PIECES[:idx]) + where
        span = pl.ds(pl.multiple_of(where * piece, piece), piece)
        rows = pl.ds(STARTS[idx], SIZES[idx])
        src = acts[idx].at[:, span] if idx < 3 else act.at[rows, span]
        return pltpu.make_async_remote_copy(src, act_got.at[rows, span], act_ssem.at[sem], act_rsem.at[sem],
                                            device_id={'tx': 1 - tx}, device_id_type=MESH)

    def columns(who, count):
        return pl.ds(pl.multiple_of(who * count, count), count)

    for copy in [att_copy] + loads:
        copy.start()
    pl.semaphore_wait(barrier, 4)
    for where in range(PIECES[0]):
        act_copy(0, where).start()
    att_copy.wait()
    o_spread = []
    for rel in (2, 3, 1):
        o_spread.append(pltpu.make_async_remote_copy(
            att_ref.at[:, columns(peer_of(rel), o_cols)], o_mine.at[columns(ty, few)], a2a_ssem.at[rel], a2a_rsem.at[rel],
            device_id={'tyz': peer_of(rel)}, device_id_type=MESH))
    for copy in o_spread:
        copy.start()
    for copy in held + weights:
        copy.start()
    o_mine[columns(ty, few), :] = att_ref[:, columns(ty, o_cols)]
    for copy in loads:
        copy.wait()
    lax.fori_loop(0, ff // 512, silu, 0)
    for copy in o_spread:
        copy.wait()
    o_copy = pltpu.make_async_remote_copy(o_mine, o_got, o_ssem, o_rsem, device_id={'tx': 1 - tx}, device_id_type=MESH)
    o_copy.start()
    for idx in (1, 2, 3):
        for where in range(PIECES[idx]):
            act_copy(idx, where).start()
    for copy in held + weights:
        copy.wait()

    def ship(rel, src, dst, ssem, rsem):
        return pltpu.make_async_remote_copy(src.at[rel], dst.at[rel], ssem.at[rel], rsem.at[rel],
                                            device_id={'tyz': peer_of(rel)}, device_id_type=MESH)

    def spread(value, src, dst, kept, ssem, rsem):
        def body(step, carry):
            rel = lax.rem(step + 2, 4)
            total = value(columns(peer_of(rel), width))

            @pl.when(rel == 0)
            def _():
                kept[...] = total

            @pl.when(rel != 0)
            def _():
                src[rel] = total.astype(BF16)
                ship(rel, src, dst, ssem, rsem).start()

            return carry

        lax.fori_loop(0, 4, body, 0)

    outs = []

    def finish(start, src, dst, kept, ssem, rsem):
        total = kept[...]
        for rel in (1, 2, 3):
            ship(rel, src, dst, ssem, rsem).wait()
        for rel in (1, 2, 3):
            total = total + dst[rel].astype(F32)
        rows = pl.ds(pl.multiple_of(start, 16), total.shape[0])
        out_ref[rows, :] = (res_ref[rows, :].astype(F32) + total).astype(out_ref.dtype)

    own = (send_own, recv_own, keep_own, own_ssem, own_rsem)
    blocks = [(src, dst, kept, row_ssem.at[idx], row_rsem.at[idx]) for idx, (src, dst, kept) in enumerate(
        ((send0, recv0, keep0), (send1, recv1, keep1), (send2, recv2, keep2), (send3, recv3, keep3)))]
    base = (1 - tx) * half
    spread(lambda cols: dot(o_mine[...], wo[:, cols]) + dot(act[...], wd[:, cols]), *own)
    for idx in range(4):
        piece = ff // PIECES[idx]
        last = PIECES[idx] - 1
        size = SIZES[idx]
        rows = slice(STARTS[idx], STARTS[idx] + size)
        if idx == 0:
            sums[:size, :] = jnp.zeros((size, sums.shape[1]), F32)
        else:
            sums[:size, :] = dot(o_got[rows, :], wo[...])

        def body(where, carry, idx=idx, piece=piece, rows=rows, size=size):
            act_copy(idx, where).wait_recv()
            span = pl.ds(pl.multiple_of(where * piece, piece), piece)
            sums[:size, :] += dot(act_got[rows, span], wd[span, :])
            return carry

        lax.fori_loop(0, last, body, 0)
        act_copy(idx, last).wait_recv()
        if idx == 0:
            finish(tx * half, *own)
            o_copy.wait_recv()
            sums[:size, :] += dot(o_got[rows, :], wo[...])
        spread(lambda cols: sums[:size, cols] + dot(act_got[rows, last * piece:], wd[last * piece:, cols]), *blocks[idx])
        if idx > 0:
            finish(base + STARTS[idx - 1], *blocks[idx - 1])
    finish(base + STARTS[3], *blocks[3])
    o_copy.wait_send()
    for idx in range(4):
        for where in range(PIECES[idx]):
            act_copy(idx, where).wait_send()
    for copy in outs:
        copy.wait()


def activation(mine, got):
    ff = mine.shape[1] // 2
    gate = (mine[:, :ff].astype(F32) + got[:, :ff].astype(F32)).astype(BF16).astype(F32)
    up = (mine[:, ff:].astype(F32) + got[:, ff:].astype(F32)).astype(BF16).astype(F32)
    return (jax.nn.silu(gate) * up).astype(BF16)


def tail(acts, got, mine, attended, w_out, w_down, residual):
    few = attended.shape[0]
    half = 4 * few
    o_cols = w_out.shape[0]
    ff, out_cols = w_down.shape
    _, width = residual.shape
    dma = pltpu.SemaphoreType.DMA
    count = sum(PIECES)
    exchange = []
    for size in (half,) + SIZES:
        exchange += [pltpu.VMEM((4, size, width), BF16), pltpu.VMEM((4, size, width), BF16), pltpu.VMEM((size, width), F32)]
    return pl.pallas_call(
        tail_kernel,
        out_shape=jax.ShapeDtypeStruct(residual.shape, residual.dtype),
        in_specs=[HBM] * 9,
        out_specs=pl.BlockSpec(memory_space=pltpu.VMEM),
        scratch_shapes=[pltpu.VMEM(attended.shape, BF16), pltpu.VMEM(residual.shape, residual.dtype), pltpu.VMEM(w_out.shape, BF16), pltpu.VMEM(w_down.shape, BF16),
                        pltpu.VMEM((SIZES[3], 2 * ff), BF16), pltpu.VMEM((SIZES[3], 2 * ff), BF16),
                        pltpu.VMEM((half, ff), BF16), pltpu.VMEM((half, ff), BF16),
                        pltpu.VMEM((half, o_cols), BF16), pltpu.VMEM((half, o_cols), BF16), pltpu.VMEM((SIZES[0], out_cols), F32),
                        pltpu.VMEM(residual.shape, residual.dtype)] + exchange
        + [dma((4,)), dma((5,)), dma, dma, dma((4,)), dma((4,)), dma((count,)), dma((count,)),
           dma((4,)), dma((4,)), dma((4, 4)), dma((4, 4)), dma((5,))],
        compiler_params=pltpu.CompilerParams(collective_id=1, has_side_effects=True, vmem_limit_bytes=50 * 2 ** 20),
        cost_estimate=pl.CostEstimate(flops=2 ** 34, bytes_accessed=2 ** 25, transcendentals=0),
        name='tail',
    )(*acts, got, mine, attended, w_out, w_down, residual)


def solution(mesh):


    row_axes = ('dp', 'tx', 'tyz')
    swap = [(0, 1), (1, 0)]

    def decode_layer(residual, ln_scale, w_query, w_key, w_value, w_gate, w_up, w_out, w_down, k_cache, v_cache, lengths):
        rows_local = k_cache.shape[0]

        def pass_on(x):
            return lax.ppermute(x, 'tx', swap)

        got, *rest = front(residual, ln_scale, w_query, w_key, w_value, w_gate, w_up, rows_local)
        gots = [got]
        for idx in range(3):
            gots.append(pass_on(rest[idx]))
        mines = rest[3:7]
        query_mine, key_new, value_new = rest[7:]
        attended, k_updated, v_updated = attend(lengths, query_mine, key_new, value_new, k_cache, v_cache)
        acts = [activation(mines[idx], gots[idx]) for idx in range(3)]
        new_resid = tail(acts, gots[3], mines[3], attended, w_out, w_down, residual)
        return new_resid, k_updated, v_updated

    in_specs = (P('dp', ('tx', 'tyz')), P(('tx', 'tyz')), P('tx', 'tyz'), P('tx', None), P('tx', None), P('tx', 'tyz'), P('tx', 'tyz'), P('tyz', 'tx'), P('tyz', 'tx'), P(row_axes, None, None), P(row_axes, None, None), P(row_axes))
    out_specs = (P('dp', ('tx', 'tyz')), P(row_axes, None, None), P(row_axes, None, None))
    return jax.shard_map(decode_layer, mesh=mesh, in_specs=in_specs, out_specs=out_specs, check_vma=False)
```

```python
import functools

import jax
import jax.numpy as jnp
import numpy as np
from jax import lax
from jax.experimental import pallas as pl
from jax.experimental.pallas import tpu as pltpu
from jax.sharding import PartitionSpec as P


LN_EPS = 1e-5
ROPE_BASE = 10000.0
MESH = pl.DeviceIdType.MESH
F32 = jnp.float32
BF16 = jnp.bfloat16
SPANS = ((0, 32), (32, 64), (96, 64), (160, 96), (256, 128), (384, 128))
CHUNKS = len(SPANS)
EARLY = 4
SLOTS = 4
WCOLS = 512
SIZES = (80, 64, 80, 32)
STARTS = (0, 80, 144, 224)
PIECES = (1, 2, 4, 4)
HBM = pl.BlockSpec(memory_space=pl.ANY)
ATTN_ROWS = 8


def front_kernel(res_in, ln_in, wq_ref, wk_ref, wv_ref, wg_ref, wu_ref,
                 got_ref, gu1_ref, gu2_ref, gu3_ref, mine0_ref, mine1_ref, mine2_ref, mine3_ref, q_ref, k_ref, v_ref,
                 res_ref, ln_ref, kv_new, raw, hn, wq, wkv, slots, stage, first, stat, stats, lnb, lns, colstat, q_send, q_got, q_own, kv_send, kv_got,
                 stat_send, stat_recv, ln_send, ln_recv, pair_send, pair_recv, x_send, x_recv, relay_send, relay_recv,
                 q_ssem, q_rsem, kv_ssem, kv_rsem, wq_sem, slot_sem, out_sem, first_ssem, first_rsem, a2a_ssem, a2a_rsem, in_sem, new_sem):
    tx = lax.axis_index('tx')
    ty = lax.axis_index('tyz')
    rows, width = res_ref.shape
    half = rows // 2
    model_dim = 8 * width
    pair = ty + 1 - 2 * lax.rem(ty, 2)
    across = lax.rem(ty + 2, 4)
    me = tx * 4 + ty
    few = k_ref.shape[0]
    dim = k_ref.shape[1]
    wcols = slots.shape[2]
    ff = wg_ref.shape[1]
    per = ff // wcols

    def dot(a, b):
        return jnp.dot(a, b, preferred_element_type=F32)

    inputs = [pltpu.make_async_copy(res_in, res_ref, in_sem.at[0]), pltpu.make_async_copy(ln_in, ln_ref, in_sem.at[1])]
    for copy in inputs:
        copy.start()
    weights = [pltpu.make_async_copy(wq_ref, wq, wq_sem.at[0]),
               pltpu.make_async_copy(wk_ref, wkv.at[:, pl.ds(0, dim)], wq_sem.at[1]),
               pltpu.make_async_copy(wv_ref, wkv.at[:, pl.ds(dim, dim)], wq_sem.at[2])]

    def fetch(ref, idx, slot):
        start = pl.multiple_of(idx * wcols, wcols)
        return pltpu.make_async_copy(ref.at[:, pl.ds(start, wcols)], slots.at[slot], slot_sem.at[slot])

    barrier = pltpu.get_barrier_semaphore()
    for off in range(1, 8):
        peer = lax.rem(me + off, 8)
        pl.semaphore_signal(barrier, inc=1, device_id={'tx': peer // 4, 'tyz': lax.rem(peer, 4)}, device_id_type=MESH)
    inputs[0].wait()
    for copy in weights:
        copy.start()
    for idx in range(SLOTS - 1):
        fetch(wg_ref, idx, idx).start()
    inputs[1].wait()
    lnb[...] = jnp.broadcast_to(ln_ref[...].astype(F32)[None, :], lnb.shape).astype(BF16)
    res = res_ref[...].astype(F32)
    row_sum = jnp.sum(res, axis=1, keepdims=True)
    row_sq = jnp.sum(jnp.square(res - row_sum / width), axis=1, keepdims=True)
    lane = lax.broadcasted_iota(jnp.int32, (rows, 128), 1)
    both = jnp.where(lax.rem(lane, 8) < 4, row_sum, row_sq).T[:8]
    sub = lax.rem(lax.broadcasted_iota(jnp.int32, (8, 128), 0), 4)
    packed = both[:, :128]
    for idx in range(1, rows // 128):
        packed = jnp.where(sub == idx, both[:, idx * 128:(idx + 1) * 128], packed)
    stat[...] = packed
    pl.semaphore_wait(barrier, 7)

    def cols(who):
        return pl.ds(pl.multiple_of(who * width, width), width)

    def actual(idx):
        start, size = SPANS[idx]
        start = (1 - tx) * half + start if start < half else tx * half + start - half
        return pl.ds(pl.multiple_of(start, 32), size)

    def block(idx):
        return pl.ds(*SPANS[idx])

    copies = []
    crossing = []
    paired = []
    relayed = []
    for idx in range(CHUNKS):
        crossing.append(pltpu.make_async_remote_copy(
            res_ref.at[actual(idx)], raw.at[block(idx), cols(ty)], x_send.at[idx], x_recv.at[idx],
            device_id={'tyz': across}, device_id_type=MESH))
        paired.append(pltpu.make_async_remote_copy(
            res_ref.at[actual(idx)], raw.at[block(idx), cols(ty)], pair_send.at[idx], pair_recv.at[idx],
            device_id={'tyz': pair}, device_id_type=MESH))
        relayed.append(pltpu.make_async_remote_copy(
            raw.at[block(idx), cols(across)], raw.at[block(idx), cols(across)], relay_send.at[idx], relay_recv.at[idx],
            device_id={'tyz': pair}, device_id_type=MESH))
    stats[me] = stat[...]
    for off in range(1, 8):
        peer = lax.rem(me + off, 8)
        copies.append(pltpu.make_async_remote_copy(
            stat, stats.at[me], stat_send.at[off], stat_recv.at[off],
            device_id={'tx': peer // 4, 'tyz': lax.rem(peer, 4)}, device_id_type=MESH))
    for off in range(1, 4):
        copies.append(pltpu.make_async_remote_copy(
            lnb, lns.at[:, cols(ty)], ln_send.at[off], ln_recv.at[off],
            device_id={'tyz': lax.rem(ty + off, 4)}, device_id_type=MESH))
    for copy in copies:
        copy.start()
    for idx in range(CHUNKS):
        crossing[idx].start()
        paired[idx].start()
    for idx in range(CHUNKS):
        raw[block(idx), cols(ty)] = res_ref[actual(idx), :]
    lns[:, cols(ty)] = lnb[...]
    for copy in copies:
        copy.wait_recv()
    total = stats[0][:4]
    for src in range(1, 8):
        total = total + stats[src][:4]
    mean = total / model_dim
    square = jnp.zeros_like(mean)
    for src in range(8):
        square = square + stats[src][4:] + width * jnp.square(stats[src][:4] / width - mean)
    scale = lax.rsqrt(square / model_dim + LN_EPS)
    upper = lax.broadcasted_iota(jnp.int32, (128, 128), 0) < 64
    for idx in range(rows // 128):
        colstat[idx * 128:(idx + 1) * 128, :] = jnp.where(upper, mean[idx:idx + 1], scale[idx:idx + 1]).T

    def norm(idx):
        centre = colstat[actual(idx), :][:, :1]
        factor = colstat[actual(idx), :][:, 64:65]
        for col in range(4):
            part = pl.ds(col * width, width)
            hn[block(idx), part] = ((raw[block(idx), part].astype(F32) - centre) * factor
                                    * lns[:1, part].astype(F32)).astype(BF16)

    q_copies = []
    for idx in range(EARLY):
        crossing[idx].wait_recv()
        relayed[idx].start()
        paired[idx].wait_recv()
        relayed[idx].wait_recv()
        norm(idx)
        if idx == 0:
            weights[0].wait()
        q_send[block(idx), :] = dot(hn[block(idx), :], wq[...]).astype(BF16)
        copy = pltpu.make_async_remote_copy(
            q_send.at[block(idx)], q_got.at[block(idx)], q_ssem.at[idx], q_rsem.at[idx],
            device_id={'tx': 1 - tx}, device_id_type=MESH)
        copy.start()
        q_copies.append(copy)
    weights[1].wait()
    weights[2].wait()
    mine_few = pl.ds(pl.multiple_of(ty * few, few), few)
    kv_send[...] = dot(hn[mine_few, :], wkv[...]).astype(BF16)
    kv_copy = pltpu.make_async_remote_copy(kv_send, kv_got, kv_ssem, kv_rsem, device_id={'tx': 1 - tx}, device_id_type=MESH)
    kv_copy.start()

    for idx in range(EARLY, CHUNKS):
        crossing[idx].wait_recv()
        relayed[idx].start()
    for idx in range(EARLY, CHUNKS):
        paired[idx].wait_recv()
        relayed[idx].wait_recv()
        norm(idx)

    outs = ((gu1_ref, STARTS[1]), (gu2_ref, STARTS[2]), (gu3_ref, STARTS[3]), (mine0_ref, half), (mine1_ref, half + STARTS[1]),
            (mine2_ref, half + STARTS[2]), (mine3_ref, half + STARTS[3]))

    def columns(step):
        return pl.ds(pl.multiple_of(step * wcols, wcols), wcols)

    def put(step, slot):
        return [pltpu.make_async_copy(stage.at[slot, pl.ds(start, out.shape[0])], out.at[:, columns(step)], out_sem.at[slot, idx])
                for idx, (out, start) in enumerate(outs)]

    def send_first(step):
        return pltpu.make_async_remote_copy(
            first.at[:, columns(step)], got_ref.at[:, columns(step)], first_ssem.at[step], first_rsem.at[step],
            device_id={'tx': 1 - tx}, device_id_type=MESH)

    def body(step, carry, gate):
        slot = lax.rem(step, SLOTS)
        side = lax.rem(step, 2)
        ahead = step + SLOTS - 1
        into = lax.rem(ahead, SLOTS)
        if gate:
            @pl.when(ahead < per)
            def _():
                fetch(wg_ref, ahead, into).start()

            @pl.when(ahead >= per)
            def _():
                fetch(wu_ref, ahead - per, into).start()

            fetch(wg_ref, 0, slot).wait()
        else:
            @pl.when(ahead < 2 * per)
            def _():
                fetch(wu_ref, ahead - per, into).start()

            fetch(wu_ref, 0, slot).wait()

        @pl.when(step >= 2)
        def _():
            for copy in put(step - 2, side):
                copy.wait()

        stage[side] = dot(hn[...], slots[slot]).astype(BF16)
        for copy in put(step, side):
            copy.start()
        first[:, columns(step)] = stage[side, :SIZES[0], :]
        send_first(step).start()
        return carry

    lax.fori_loop(0, per, functools.partial(body, gate=True), 0)
    q_own[...] = dot(hn[half:, :], wq[...]).astype(BF16)
    own_few = pl.ds(pl.multiple_of(half + ty * few, few), few)
    kv_own = dot(hn[own_few, :], wkv[...])
    kv_copy.wait()
    kv = (kv_own + kv_got[...].astype(F32)).astype(BF16)
    kv_new[0] = kv[:, :dim]
    kv_new[1] = kv[:, dim:]
    for copy in q_copies:
        copy.wait()
    q_own[...] = (q_own[...].astype(F32) + q_got[...].astype(F32)).astype(BF16)
    news = [pltpu.make_async_copy(kv_new.at[0], k_ref, new_sem.at[0]), pltpu.make_async_copy(kv_new.at[1], v_ref, new_sem.at[1]),
            pltpu.make_async_copy(q_own.at[mine_few], q_ref.at[ty], new_sem.at[2])]
    spread = []
    for off in (2, 1, 3):
        peer = lax.rem(ty + off, 4)
        spread.append(pltpu.make_async_remote_copy(
            q_own.at[pl.ds(pl.multiple_of(peer * few, few), few)], q_ref.at[ty], a2a_ssem.at[off], a2a_rsem.at[off],
            device_id={'tyz': peer}, device_id_type=MESH))
    for copy in spread + news:
        copy.start()
    lax.fori_loop(per, 2 * per, functools.partial(body, gate=False), 0)
    for copy in spread + news:
        copy.wait()
    for copy in copies + crossing + paired + relayed:
        copy.wait_send()
    for step in (2 * per - 2, 2 * per - 1):
        for copy in put(step, step % 2):
            copy.wait()
    for step in range(2 * per):
        send_first(step).wait()


def front(residual, ln_scale, w_query, w_key, w_value, w_gate, w_up, few):
    rows, width = residual.shape
    half = rows // 2
    depth, q_cols = w_query.shape
    dim = w_key.shape[1]
    ff = w_gate.shape[1]
    dma = pltpu.SemaphoreType.DMA
    shape = jax.ShapeDtypeStruct
    blocks = tuple(shape((size, 2 * ff), BF16) for size in SIZES)
    return pl.pallas_call(
        front_kernel,
        out_shape=blocks + blocks + (shape((4, few, q_cols), BF16), shape((few, dim), BF16), shape((few, dim), BF16)),
        in_specs=[HBM] * 7,
        out_specs=(HBM,) * 11,
        scratch_shapes=[
            pltpu.VMEM((rows, width), BF16), pltpu.VMEM((width,), BF16), pltpu.VMEM((2, few, dim), BF16),
            pltpu.VMEM((rows, depth), BF16), pltpu.VMEM((rows, depth), BF16),
            pltpu.VMEM((depth, q_cols), BF16), pltpu.VMEM((depth, 2 * dim), BF16),
            pltpu.VMEM((SLOTS, depth, WCOLS), BF16), pltpu.VMEM((2, rows, WCOLS), BF16), pltpu.VMEM((SIZES[0], 2 * ff), BF16),
            pltpu.VMEM((8, 128), F32), pltpu.VMEM((8, 8, 128), F32),
            pltpu.VMEM((16, width), BF16), pltpu.VMEM((16, depth), BF16), pltpu.VMEM((rows, 128), F32),
            pltpu.VMEM((half, q_cols), BF16), pltpu.VMEM((half, q_cols), BF16), pltpu.VMEM((half, q_cols), BF16),
            pltpu.VMEM((few, 2 * dim), BF16), pltpu.VMEM((few, 2 * dim), BF16),
            dma((8,)), dma((8,)), dma((4,)), dma((4,)), dma((CHUNKS,)), dma((CHUNKS,)), dma((CHUNKS,)), dma((CHUNKS,)),
            dma((CHUNKS,)), dma((CHUNKS,)), dma((CHUNKS,)), dma((CHUNKS,)), dma, dma, dma((3,)), dma((SLOTS,)), dma((2, 7)),
            dma((2 * ff // WCOLS,)), dma((2 * ff // WCOLS,)), dma((4,)), dma((4,)), dma((2,)), dma((3,))],
        compiler_params=pltpu.CompilerParams(collective_id=0, has_side_effects=True),
        cost_estimate=pl.CostEstimate(flops=2 ** 34, bytes_accessed=2 ** 26, transcendentals=0),
        name='front',
    )(residual, ln_scale, w_query, w_key, w_value, w_gate, w_up)


def attend_kernel(len_ref, freq_ref, q_ref, knew_ref, vnew_ref, kc_ref, vc_ref, o_ref, kout_ref, vout_ref, q_low, q_high, k_rot, v_new, o_low, o_high):
    step = pl.program_id(0)
    groups, rows, span = q_ref.shape
    seq, dim = kc_ref.shape[1:]
    heads = groups * span // dim
    half = dim // 2
    sub = lax.broadcasted_iota(jnp.int32, (rows, 1), 0)
    positions = jnp.zeros((rows, 1), jnp.int32)
    for row in range(rows):
        positions = jnp.where(sub == row, len_ref[step * rows + row], positions)
    angles = positions.astype(F32) * freq_ref[...]
    cos_part = jnp.cos(angles)
    sin_part = jnp.sin(angles)

    def rotate(first, second):
        first = first.astype(F32)
        second = second.astype(F32)
        return first * cos_part - second * sin_part, second * cos_part + first * sin_part

    k_rot[:, :half], k_rot[:, half:] = rotate(knew_ref[:, :half], knew_ref[:, half:])
    v_new[...] = vnew_ref[...].astype(F32)
    for head in range(heads):
        group, start = divmod(head * dim, span)
        place = pl.ds(head * rows, rows)
        q_low[place, :], q_high[place, :] = rotate(q_ref[group, :, start:start + half], q_ref[group, :, start + half:start + dim])
    for row in range(rows):
        pos = len_ref[step * rows + row]
        start = pl.multiple_of((pos // 16) * 16, 16)
        hit = lax.broadcasted_iota(jnp.int32, (16, 1), 0) == pos - start
        for cache, new, out in ((kc_ref, k_rot, kout_ref), (vc_ref, v_new, vout_ref)):
            out[row] = cache[row]
            window = cache[row, pl.ds(start, 16), :].astype(F32)
            out[row, pl.ds(start, 16), :] = jnp.where(hit, new[row:row + 1, :], window).astype(BF16)
    for row in range(rows):
        pos = len_ref[step * rows + row]
        place = pl.ds(row, heads, stride=rows)
        query = jnp.concatenate([q_low[place, :], q_high[place, :]], axis=1).astype(BF16)
        scores = lax.dot_general(query, kout_ref[row], (((1,), (1,)), ((), ())), preferred_element_type=F32) * dim ** -0.5
        where = lax.broadcasted_iota(jnp.int32, (1, seq), 1) <= pos
        scores = jnp.where(where, scores, -1e30)
        top = jnp.max(scores, axis=1, keepdims=True)
        weight = jnp.exp(scores - top)
        probs = (weight / jnp.sum(weight, axis=1, keepdims=True)).astype(BF16)
        total = jnp.dot(probs, vout_ref[row], preferred_element_type=F32)
        o_low[place, :] = total[:, :half]
        o_high[place, :] = total[:, half:]
    for head in range(heads):
        o_ref[:, head * dim:head * dim + half] = o_low[head * rows:(head + 1) * rows, :].astype(BF16)
        o_ref[:, head * dim + half:(head + 1) * dim] = o_high[head * rows:(head + 1) * rows, :].astype(BF16)


def attend(lengths, query, key_new, value_new, k_cache, v_cache):
    groups, rows, span = query.shape
    seq, dim = k_cache.shape[1:]
    width = groups * span
    freq = jnp.asarray(np.power(ROPE_BASE, -2.0 * np.arange(dim // 2) / dim)[None, :].astype(np.float32))
    new = pl.BlockSpec((ATTN_ROWS, dim), lambda i, lens: (i, 0))
    big = pl.BlockSpec((ATTN_ROWS, seq, dim), lambda i, lens: (i, 0, 0))
    return pl.pallas_call(
        attend_kernel,
        grid_spec=pltpu.PrefetchScalarGridSpec(
            num_scalar_prefetch=1, grid=(rows // ATTN_ROWS,),
            in_specs=[pl.BlockSpec((1, dim // 2), lambda i, lens: (0, 0)),
                      pl.BlockSpec((groups, ATTN_ROWS, span), lambda i, lens: (0, i, 0)), new, new, big, big],
            out_specs=[pl.BlockSpec((ATTN_ROWS, width), lambda i, lens: (i, 0)), big, big],
            scratch_shapes=[pltpu.VMEM((ATTN_ROWS * width // dim, dim // 2), F32)] * 2 + [pltpu.VMEM((ATTN_ROWS, dim), F32)] * 2
            + [pltpu.VMEM((ATTN_ROWS * width // dim, dim // 2), F32)] * 2),
        out_shape=(jax.ShapeDtypeStruct((rows, width), BF16),
                   jax.ShapeDtypeStruct(k_cache.shape, BF16),
                   jax.ShapeDtypeStruct(v_cache.shape, BF16)),
        compiler_params=pltpu.CompilerParams(vmem_limit_bytes=67043328),
        cost_estimate=pl.CostEstimate(flops=2 ** 33, bytes_accessed=2 ** 27, transcendentals=2 ** 20),
        name='attend',
    )(lengths, freq, query, key_new, value_new, k_cache, v_cache)


def tail_kernel(act0_ref, act1_ref, act2_ref, got_ref, mine_ref, att_in, wo_ref, wd_ref, res_in, out_ref,
                att_ref, res_ref, wo, wd, gu_got, gu_mine, act, act_got, o_mine, o_got, sums, out_buf,
                send_own, recv_own, keep_own, send0, recv0, keep0, send1, recv1, keep1, send2, recv2, keep2, send3, recv3, keep3,
                w_sem, gu_sem, o_ssem, o_rsem, a2a_ssem, a2a_rsem, act_ssem, act_rsem, own_ssem, own_rsem, row_ssem, row_rsem, out_sem):
    tx = lax.axis_index('tx')
    ty = lax.axis_index('tyz')
    few = att_ref.shape[0]
    half = 4 * few
    width = out_ref.shape[1]
    ff = act.shape[1]
    o_cols = o_mine.shape[1]
    acts = (act0_ref, act1_ref, act2_ref)

    def dot(a, b):
        return jnp.dot(a, b, preferred_element_type=F32)

    def peer_of(rel):
        return 2 * lax.rem(ty // 2 + rel // 2, 2) + lax.rem(lax.rem(ty, 2) + lax.rem(rel, 2), 2)

    weights = [pltpu.make_async_copy(wo_ref, wo, w_sem.at[0]), pltpu.make_async_copy(wd_ref, wd, w_sem.at[1]),
               pltpu.make_async_copy(res_in, res_ref, w_sem.at[2])]
    att_copy = pltpu.make_async_copy(att_in, att_ref, w_sem.at[3])
    loads = [pltpu.make_async_copy(mine_ref, gu_mine, gu_sem.at[3]), pltpu.make_async_copy(got_ref, gu_got, gu_sem.at[4])]
    held = [pltpu.make_async_copy(ref, act.at[pl.ds(STARTS[idx], SIZES[idx])], gu_sem.at[idx]) for idx, ref in enumerate(acts)]
    barrier = pltpu.get_barrier_semaphore()
    pl.semaphore_signal(barrier, inc=1, device_id={'tx': 1 - tx}, device_id_type=MESH)
    for rel in (1, 2, 3):
        pl.semaphore_signal(barrier, inc=1, device_id={'tyz': peer_of(rel)}, device_id_type=MESH)

    def silu(col, carry):
        part = pl.ds(pl.multiple_of(col * 512, 512), 512)
        other = pl.ds(pl.multiple_of(ff + col * 512, 512), 512)
        gate = (gu_mine[:, part].astype(F32) + gu_got[:, part].astype(F32)).astype(BF16).astype(F32)
        up = (gu_mine[:, other].astype(F32) + gu_got[:, other].astype(F32)).astype(BF16).astype(F32)
        act[STARTS[3]:, part] = (gate / (1.0 + jnp.exp(-gate)) * up).astype(BF16)
        return carry

    def act_copy(idx, where):
        piece = ff // PIECES[idx]
        sem = sum(PIECES[:idx]) + where
        span = pl.ds(pl.multiple_of(where * piece, piece), piece)
        rows = pl.ds(STARTS[idx], SIZES[idx])
        src = acts[idx].at[:, span] if idx < 3 else act.at[rows, span]
        return pltpu.make_async_remote_copy(src, act_got.at[rows, span], act_ssem.at[sem], act_rsem.at[sem],
                                            device_id={'tx': 1 - tx}, device_id_type=MESH)

    def columns(who, count):
        return pl.ds(pl.multiple_of(who * count, count), count)

    for copy in [att_copy] + loads:
        copy.start()
    pl.semaphore_wait(barrier, 4)
    for where in range(PIECES[0]):
        act_copy(0, where).start()
    att_copy.wait()
    o_spread = []
    for rel in (2, 3, 1):
        o_spread.append(pltpu.make_async_remote_copy(
            att_ref.at[:, columns(peer_of(rel), o_cols)], o_mine.at[columns(ty, few)], a2a_ssem.at[rel], a2a_rsem.at[rel],
            device_id={'tyz': peer_of(rel)}, device_id_type=MESH))
    for copy in o_spread:
        copy.start()
    for copy in held + weights:
        copy.start()
    o_mine[columns(ty, few), :] = att_ref[:, columns(ty, o_cols)]
    for copy in loads:
        copy.wait()
    lax.fori_loop(0, ff // 512, silu, 0)
    for copy in o_spread:
        copy.wait()
    o_copy = pltpu.make_async_remote_copy(o_mine, o_got, o_ssem, o_rsem, device_id={'tx': 1 - tx}, device_id_type=MESH)
    o_copy.start()
    for idx in (1, 2, 3):
        for where in range(PIECES[idx]):
            act_copy(idx, where).start()
    for copy in held + weights:
        copy.wait()

    def ship(rel, src, dst, ssem, rsem):
        return pltpu.make_async_remote_copy(src.at[rel], dst.at[rel], ssem.at[rel], rsem.at[rel],
                                            device_id={'tyz': peer_of(rel)}, device_id_type=MESH)

    def spread(value, src, dst, kept, ssem, rsem, unroll=1):
        def body(step, carry):
            rel = lax.rem(step + 2, 4)
            total = value(columns(peer_of(rel), width))

            @pl.when(rel == 0)
            def _():
                kept[...] = total

            @pl.when(rel != 0)
            def _():
                src[rel] = total.astype(BF16)
                ship(rel, src, dst, ssem, rsem).start()

            return carry

        lax.fori_loop(0, 4, body, 0, unroll=unroll)

    outs = []

    def finish(start, src, dst, kept, ssem, rsem):
        total = kept[...]
        for rel in (1, 2, 3):
            ship(rel, src, dst, ssem, rsem).wait()
        for rel in (1, 2, 3):
            total = total + dst[rel].astype(F32)
        rows = pl.ds(pl.multiple_of(start, 16), total.shape[0])
        out_ref[rows, :] = (res_ref[rows, :].astype(F32) + total).astype(out_ref.dtype)

    own = (send_own, recv_own, keep_own, own_ssem, own_rsem)
    blocks = [(src, dst, kept, row_ssem.at[idx], row_rsem.at[idx]) for idx, (src, dst, kept) in enumerate(
        ((send0, recv0, keep0), (send1, recv1, keep1), (send2, recv2, keep2), (send3, recv3, keep3)))]
    base = (1 - tx) * half
    spread(lambda cols: dot(o_mine[...], wo[:, cols]) + dot(act[...], wd[:, cols]), *own)
    for idx in range(4):
        piece = ff // PIECES[idx]
        last = PIECES[idx] - 1
        size = SIZES[idx]
        rows = slice(STARTS[idx], STARTS[idx] + size)
        if idx == 0:
            sums[:size, :] = jnp.zeros((size, sums.shape[1]), F32)
        else:
            sums[:size, :] = dot(o_got[rows, :], wo[...])

        def body(where, carry, idx=idx, piece=piece, rows=rows, size=size):
            act_copy(idx, where).wait_recv()
            span = pl.ds(pl.multiple_of(where * piece, piece), piece)
            sums[:size, :] += dot(act_got[rows, span], wd[span, :])
            return carry

        lax.fori_loop(0, last, body, 0)
        act_copy(idx, last).wait_recv()
        if idx == 0:
            finish(tx * half, *own)
            o_copy.wait_recv()
            sums[:size, :] += dot(o_got[rows, :], wo[...])
        spread(lambda cols: sums[:size, cols] + dot(act_got[rows, last * piece:], wd[last * piece:, cols]), *blocks[idx], unroll=4 if idx == 3 else 1)
        if idx > 0:
            finish(base + STARTS[idx - 1], *blocks[idx - 1])
    finish(base + STARTS[3], *blocks[3])
    o_copy.wait_send()
    for idx in range(4):
        for where in range(PIECES[idx]):
            act_copy(idx, where).wait_send()
    for copy in outs:
        copy.wait()


def activation(mine, got):
    ff = mine.shape[1] // 2
    gate = (mine[:, :ff].astype(F32) + got[:, :ff].astype(F32)).astype(BF16).astype(F32)
    up = (mine[:, ff:].astype(F32) + got[:, ff:].astype(F32)).astype(BF16).astype(F32)
    return (jax.nn.silu(gate) * up).astype(BF16)


def tail(acts, got, mine, attended, w_out, w_down, residual):
    few = attended.shape[0]
    half = 4 * few
    o_cols = w_out.shape[0]
    ff, out_cols = w_down.shape
    _, width = residual.shape
    dma = pltpu.SemaphoreType.DMA
    count = sum(PIECES)
    exchange = []
    for size in (half,) + SIZES:
        exchange += [pltpu.VMEM((4, size, width), BF16), pltpu.VMEM((4, size, width), BF16), pltpu.VMEM((size, width), F32)]
    return pl.pallas_call(
        tail_kernel,
        out_shape=jax.ShapeDtypeStruct(residual.shape, residual.dtype),
        in_specs=[HBM] * 9,
        out_specs=pl.BlockSpec(memory_space=pltpu.VMEM),
        scratch_shapes=[pltpu.VMEM(attended.shape, BF16), pltpu.VMEM(residual.shape, residual.dtype), pltpu.VMEM(w_out.shape, BF16), pltpu.VMEM(w_down.shape, BF16),
                        pltpu.VMEM((SIZES[3], 2 * ff), BF16), pltpu.VMEM((SIZES[3], 2 * ff), BF16),
                        pltpu.VMEM((half, ff), BF16), pltpu.VMEM((half, ff), BF16),
                        pltpu.VMEM((half, o_cols), BF16), pltpu.VMEM((half, o_cols), BF16), pltpu.VMEM((SIZES[0], out_cols), F32),
                        pltpu.VMEM(residual.shape, residual.dtype)] + exchange
        + [dma((4,)), dma((5,)), dma, dma, dma((4,)), dma((4,)), dma((count,)), dma((count,)),
           dma((4,)), dma((4,)), dma((4, 4)), dma((4, 4)), dma((5,))],
        compiler_params=pltpu.CompilerParams(collective_id=1, has_side_effects=True, vmem_limit_bytes=50 * 2 ** 20),
        cost_estimate=pl.CostEstimate(flops=2 ** 34, bytes_accessed=2 ** 25, transcendentals=0),
        name='tail',
    )(*acts, got, mine, attended, w_out, w_down, residual)


def solution(mesh):


    row_axes = ('dp', 'tx', 'tyz')
    swap = [(0, 1), (1, 0)]

    def decode_layer(residual, ln_scale, w_query, w_key, w_value, w_gate, w_up, w_out, w_down, k_cache, v_cache, lengths):
        rows_local = k_cache.shape[0]

        def pass_on(x):
            return lax.ppermute(x, 'tx', swap)

        got, *rest = front(residual, ln_scale, w_query, w_key, w_value, w_gate, w_up, rows_local)
        gots = [got]
        for idx in range(3):
            gots.append(pass_on(rest[idx]))
        mines = rest[3:7]
        query_mine, key_new, value_new = rest[7:]
        attended, k_updated, v_updated = attend(lengths, query_mine, key_new, value_new, k_cache, v_cache)
        acts = [activation(mines[idx], gots[idx]) for idx in range(3)]
        new_resid = tail(acts, gots[3], mines[3], attended, w_out, w_down, residual)
        return new_resid, k_updated, v_updated

    in_specs = (P('dp', ('tx', 'tyz')), P(('tx', 'tyz')), P('tx', 'tyz'), P('tx', None), P('tx', None), P('tx', 'tyz'), P('tx', 'tyz'), P('tyz', 'tx'), P('tyz', 'tx'), P(row_axes, None, None), P(row_axes, None, None), P(row_axes))
    out_specs = (P('dp', ('tx', 'tyz')), P(row_axes, None, None), P(row_axes, None, None))
    return jax.shard_map(decode_layer, mesh=mesh, in_specs=in_specs, out_specs=out_specs, check_vma=False)
```
